32 devices in a mesh: slab: 8 (over z, y), chan: 4 (over x, core).
Axes of the slice: x: 2, y: 2, z: 4, core: 2. Of those that a mesh axis runs over, the one named last changes fastest.
Arguments:
- saved_input: float32 [512, 48, 256], P('chan', 'slab'), may hold values from -6 to 6
- pre_first: float32 [512, 48, 256], P('chan', 'slab'), may hold values from -8 to 8
- pre_second: float32 [512, 48, 256], P('chan', 'slab'), may hold values from -8 to 8
- out_grad: float32 [512, 48, 256], P('chan', 'slab'), may hold values from -12 to 12
- weight_first: float32 [27, 512, 512], P(None, 'chan'), may hold values from -0.0546875 to 0.0546875
- weight_second: float32 [27, 512, 512], P(None, 'chan'), may hold values from -0.0546875 to 0.0546875
Outputs:
- input_grad: float32 [512, 48, 256], P('chan', 'slab')
- grad_weight_first: float32 [27, 512, 512], P(None, 'chan', 'slab')
- grad_weight_second: float32 [27, 512, 512], P(None, 'chan', 'slab')
The draws below stay inside these ranges and needn't reach their ends.
All inputs are finite; a program needn't handle non-finite values.
Results may differ from the reference program's by a relative error of at most 0.00013.
Values sent between devices are 32-bit elements; how exact they have to be, the bound alone decides.
A program may use at most 320 MiB of HBM per device.

```python
import math
import jax
import jax.numpy as jnp
from jax import lax

C = 512
TAPS = 27
AREA = 256
PLANES = 48


def with_spikes(result, stream_key, source, target, blocks, factor):
    def block_of(axis_at):
        return (jnp.arange(result.shape[axis_at]) // (result.shape[axis_at] // blocks)).reshape((-1,) + (1,) * (result.ndim - 1 - axis_at))

    first = jax.random.permutation(stream_key, blocks)[block_of(target)]
    other_side = (block_of(target) + blocks // 2) % blocks
    return jnp.where((block_of(source) == first) | (block_of(source) == other_side), factor * result, result)


def block_scale(own_key, dims, shards, least, high):
    level = 1.0
    for position, blocks in shards:
        steps = jax.random.uniform(jax.random.fold_in(jax.random.fold_in(own_key, 6), position), (blocks,), jnp.float32, least / len(shards), high / len(shards))
        level = level * jnp.repeat(jnp.exp(steps), dims[position] // blocks).reshape((-1,) + (1,) * (len(dims) - 1 - position))
    return level


def scatter_about(rng, shape, scale, limit, split=(), kind=jnp.bfloat16):
    gain = block_scale(rng, shape, split, -0.22, 0.18) if split else 1.0
    array = jax.random.normal(rng, shape, jnp.float32) * scale * gain
    return jnp.minimum(jnp.maximum(array, -limit), limit).astype(kind)


def gaussian_with(stream_key, shape, width, reach, shards, heavy, dtype=jnp.bfloat16):
    drawn = width * jax.random.normal(stream_key, shape, jnp.float32)
    if shards:
        drawn = drawn * block_scale(stream_key, shape, shards, -0.22, 0.18)
    return jnp.clip(with_spikes(drawn, jax.random.fold_in(stream_key, 3), *heavy), -reach, reach).astype(dtype)


def setup_inputs(seed: int = 0) -> dict:
    splits = jax.random.split(jax.random.key(seed), 7)
    saved_input = scatter_about(splits[0], (C, PLANES, AREA), 1.0, 6.0, ((0, 4), (1, 8)), jnp.float32)
    pre_first = scatter_about(splits[1], (C, PLANES, AREA), 1.5, 8.0, ((0, 4), (1, 8)), jnp.float32)
    pre_second = scatter_about(splits[2], (C, PLANES, AREA), 1.5, 8.0, ((0, 4), (1, 8)), jnp.float32)
    out_grad = gaussian_with(splits[3], (C, PLANES, AREA), 2.0, 12.0, ((0, 4), (1, 8)), (1, 0, 8, 2.0), jnp.float32)
    weight_first = scatter_about(splits[4], (TAPS, C, C), (27 * C) ** -0.5, 0.0546875, ((1, 4),), jnp.float32)
    weight_second = scatter_about(splits[5], (TAPS, C, C), (27 * C) ** -0.5, 0.0546875, ((1, 4),), jnp.float32)
    return {"saved_input": saved_input, "pre_first": pre_first, "pre_second": pre_second, "out_grad": out_grad, "weight_first": weight_first, "weight_second": weight_second}


OFFSETS = [(depth_step, row_step, col_step) for depth_step in (-1, 0, 1) for row_step in (-1, 0, 1) for col_step in (-1, 0, 1)]

def silu_slope(values):
    sigma = jax.nn.sigmoid(values)
    return sigma * (1.0 + values * (1.0 - sigma))

def layer_back(layer_input, grad_out, weight):
    channels, planes, area_cells = layer_input.shape
    side_len = math.isqrt(area_cells)
    widths = ((0, 0), (1, 1), (1, 1), (1, 1))
    input_pad = jnp.pad(layer_input.reshape(channels, planes, side_len, side_len), widths)
    grad_pad = jnp.pad(grad_out.reshape(channels, planes, side_len, side_len), widths)
    grad_flat = grad_out.reshape(channels, planes * area_cells)
    grad_in = jnp.zeros((channels, planes * area_cells), jnp.float32)
    weight_rows = []
    for tap_index, (depth_step, row_step, col_step) in enumerate(OFFSETS):
        grad_shift = grad_pad[:, 1 - depth_step:1 - depth_step + planes, 1 - row_step:1 - row_step + side_len, 1 - col_step:1 - col_step + side_len]
        grad_in = grad_in + jnp.dot(weight[tap_index], grad_shift.reshape(channels, -1), precision=lax.Precision.HIGHEST, preferred_element_type=jnp.float32)
        input_shift = input_pad[:, 1 + depth_step:1 + depth_step + planes, 1 + row_step:1 + row_step + side_len, 1 + col_step:1 + col_step + side_len]
        weight_rows.append(lax.dot_general(input_shift.reshape(channels, -1), grad_flat, (((1,), (1,)), ((), ())), precision=lax.Precision.HIGHEST, preferred_element_type=jnp.float32))
    grad_weight = jnp.stack(weight_rows, 0) / math.sqrt(planes * area_cells)
    return (grad_in.reshape(channels, planes, area_cells), grad_weight)

def reference(saved_input, pre_first, pre_second, out_grad, weight_first, weight_second):
    hidden = jax.nn.silu(pre_first)
    second_grad = out_grad * silu_slope(pre_second)
    hidden_grad, grad_weight_second = layer_back(hidden, second_grad, weight_second)
    first_grad = hidden_grad * silu_slope(pre_first)
    input_grad, grad_weight_first = layer_back(saved_input, first_grad, weight_first)
    return (input_grad, grad_weight_first, grad_weight_second)
```

```python
import functools
import math

import jax
import jax.numpy as jnp
from jax import lax
from jax.experimental import pallas as pl
from jax.experimental.pallas import tpu as pltpu
from jax.sharding import PartitionSpec as P

F32 = jnp.float32
BF16 = jnp.bfloat16
MESH = pl.DeviceIdType.MESH
STEPS = (-1, 0, 1)
IN_PLANE = [(row_step, col_step) for row_step in STEPS for col_step in STEPS]


def silu_slope(values):
    sigma = jax.nn.sigmoid(values)
    return sigma * (1.0 + values * (1.0 - sigma))


def halves(value):
    high = value.astype(BF16)
    return high, (value - high.astype(F32)).astype(BF16)


def dot_nn(left, right):
    return lax.dot_general(left, right, (((1,), (0,)), ((), ())), preferred_element_type=F32)


def dot_nt(left, right):
    return lax.dot_general(left, right, (((1,), (1,)), ((), ())), preferred_element_type=F32)


def mega(
    dims,
    second_ref, hidden_ref, saved_ref, slope_ref, weight2_ref, weight1_ref,
    grad_ref, out1_ref, out2_ref,
    full, full_h, full_l, moved_h, moved_l, taps_h, taps_l, stage, raw, mixed,
    part2, part1, got2, got1,
    stage_sem, gather_send, gather_recv, rim_send, rim_recv, ring_send, ring_recv, free_sem,
):
    slabs, chans, total, planes, area, side = dims
    channels = total // chans
    block = total // slabs
    groups = 128 // block
    rows = len(IN_PLANE) * channels // groups
    cut = -(-rows // 16) * 8
    slices = ((0, cut), (cut, rows - cut))
    chips = chans // 2
    width = planes * area
    third = 3 * channels

    slab = lax.axis_index("slab")
    chan = lax.axis_index("chan")
    chip, core = chan // 2, chan % 2
    odd = slab % 2
    place = (1 - odd) * (slab // 2) + odd * (slabs - 1 - slab // 2)

    def slab_at(spot):
        upper = spot // (slabs // 2)
        return (1 - upper) * 2 * spot + upper * (2 * (slabs - 1 - spot) + 1)

    ring_next = slab_at((place + 1) % slabs)
    ring_prev = slab_at((place + slabs - 1) % slabs)
    partner = chip * 2 + 1 - core

    def far_chan(j):
        return ((chip + j) % chips) * 2 + core

    def near_chan(j):
        return ((chip + chips - j) % chips) * 2 + core

    has_left = slab > 0
    has_right = slab < slabs - 1
    rims = jnp.minimum(slab, 1) + jnp.minimum(slabs - 1 - slab, 1)

    def tell(semaphore):
        for j in range(1, chips):
            pl.semaphore_signal(semaphore, inc=1, device_id={"chan": far_chan(j)}, device_id_type=MESH)
        pl.semaphore_signal(semaphore, inc=1, device_id={"chan": partner}, device_id_type=MESH)

        @pl.when(has_left)
        def _():
            pl.semaphore_signal(semaphore, inc=1, device_id={"slab": slab - 1}, device_id_type=MESH)

        @pl.when(has_right)
        def _():
            pl.semaphore_signal(semaphore, inc=1, device_id={"slab": slab + 1}, device_id_type=MESH)

    barrier = pltpu.get_barrier_semaphore()
    tell(barrier)
    pl.semaphore_signal(barrier, inc=1, device_id={"slab": ring_next}, device_id_type=MESH)
    pl.semaphore_signal(barrier, inc=1, device_id={"slab": ring_prev}, device_id_type=MESH)
    pl.semaphore_wait(barrier, 2 + chips + rims)

    def chan_rows(index):
        return pl.ds(pl.multiple_of(index * channels, channels), channels)

    def lanes(slot, count=1):
        return pl.ds(pl.multiple_of(slot * area, area), count * area)

    mine = chan_rows(chan)

    def stage_copy(weight_ref, depth):
        return pltpu.make_async_copy(weight_ref.at[depth], stage, stage_sem.at[0])

    def rim_copy(layer, toward, source):
        slot = (0, planes + 1)[toward]
        target = (slab + 1, slab - 1)[toward]
        return pltpu.make_async_remote_copy(
            src_ref=source,
            dst_ref=full.at[mine, lanes(slot)],
            send_sem=rim_send.at[layer, toward],
            recv_sem=rim_recv.at[layer, toward],
            device_id={"slab": target},
            device_id_type=MESH,
        )

    def gather_copy(layer, slot, source, where, index, target):
        return pltpu.make_async_remote_copy(
            src_ref=source,
            dst_ref=full.at[where, lanes(slot)],
            send_sem=gather_send.at[layer, slot, index],
            recv_sem=gather_recv.at[layer, slot, index],
            device_id={"chan": target},
            device_id_type=MESH,
        )

    def gather_start(layer, slot, source):
        for j in range(1, chips):
            gather_copy(layer, slot, source, mine, j, far_chan(j)).start()
        gather_copy(layer, slot, source, mine, 0, partner).start()

    def gather_forward(layer, slot):
        for j in range(1, chips):
            where = chan_rows(near_chan(j))
            view = full.at[where, lanes(slot)]
            gather_copy(layer, slot, view, where, j, partner).wait_recv()
            gather_copy(layer, slot, view, where, chips + j, partner).start()

    def gather_finish(layer, slot):
        where = chan_rows(partner)
        gather_copy(layer, slot, full.at[where, lanes(slot)], where, 0, partner).wait_recv()
        for j in range(1, chips):
            where = chan_rows(((chip + chips - j) % chips) * 2 + 1 - core)
            gather_copy(layer, slot, full.at[where, lanes(slot)], where, chips + j, partner).wait_recv()

    def gather_sent(layer, slot):
        view = full.at[mine, lanes(slot)]
        for index in [*range(chips), *range(chips + 1, 2 * chips)]:
            gather_copy(layer, slot, view, mine, index, partner).wait_send()

    def rim_ends(layer, action):
        @pl.when(has_left)
        def _():
            action(0)

        @pl.when(has_right)
        def _():
            action(planes + 1)

    def rim_gather(layer):
        @pl.when(has_left)
        def _():
            rim_copy(layer, 0, full.at[mine, lanes(0)]).wait_recv()
            gather_start(layer, 0, full.at[mine, lanes(0)])

        @pl.when(has_right)
        def _():
            rim_copy(layer, 1, full.at[mine, lanes(planes + 1)]).wait_recv()
            gather_start(layer, planes + 1, full.at[mine, lanes(planes + 1)])

    def rim_sent(layer):
        @pl.when(has_right)
        def _():
            rim_copy(layer, 0, full.at[mine, lanes(0)]).wait_send()

        @pl.when(has_left)
        def _():
            rim_copy(layer, 1, full.at[mine, lanes(0)]).wait_send()

    def split_full(slot):
        @pl.loop(0, total // 32)
        def _(index):
            where = pl.ds(pl.multiple_of(index * 32, 32), 32)
            high, low = halves(full[where, lanes(slot)])
            full_h[where, lanes(slot)] = high
            full_l[where, lanes(slot)] = low

    def zero_slot(slot):
        @pl.loop(0, total // 32)
        def _(index):
            where = pl.ds(pl.multiple_of(index * 32, 32), 32)
            full_h[where, lanes(slot)] = jnp.zeros((32, area), BF16)
            full_l[where, lanes(slot)] = jnp.zeros((32, area), BF16)

    def split_all():
        @pl.loop(1, planes + 1)
        def _(slot):
            split_full(slot)

        @pl.when(has_left)
        def _():
            split_full(0)

        @pl.when(slab == 0)
        def _():
            zero_slot(0)

        @pl.when(has_right)
        def _():
            split_full(planes + 1)

        @pl.when(slab == slabs - 1)
        def _():
            zero_slot(planes + 1)

    cells = lax.broadcasted_iota(jnp.int32, (1, area), 1)
    row_ids, col_ids = cells // side, cells % side

    def mask_of(row_step, col_step):
        valid = (
            (row_ids + row_step >= 0)
            & (row_ids + row_step < side)
            & (col_ids + col_step >= 0)
            & (col_ids + col_step < side)
        )
        return jnp.where(valid, 1.0, 0.0).astype(F32)

    def shifted(value, row_step, col_step):
        if row_step == 0 and col_step == 0:
            return value
        shift = (-(row_step * side + col_step)) % area
        return pltpu.roll(value, shift, 1) * mask_of(row_step, col_step)

    def build_moved(source):
        @pl.loop(0, planes)
        def _(plane):
            @pl.loop(0, channels // 32)
            def _(index):
                start = pl.multiple_of(index * 32, 32)
                value = source[pl.ds(start, 32), lanes(plane)]
                for tap, (row_step, col_step) in enumerate(IN_PLANE):
                    high, low = halves(shifted(value, row_step, col_step))
                    where = pl.ds(pl.multiple_of(tap * channels + start, 32), 32)
                    moved_h[where, lanes(plane)] = high
                    moved_l[where, lanes(plane)] = low

    def split_taps(weight_ref):
        for depth in range(3):
            stage_copy(weight_ref, depth).wait()

            @pl.loop(0, 9 * channels // 48)
            def _(index):
                where = pl.ds(pl.multiple_of(index * 48, 48), 48)
                high, low = halves(stage[where, :])
                taps_h[depth, where, :] = high
                taps_l[depth, where, :] = low

            if depth < 2:
                stage_copy(weight_ref, depth + 1).start()

    parts = (part2, part1)
    gots = (got2, got1)
    outs = (out2_ref, out1_ref)

    def ring_copy(layer, flow, step, way, owner):
        span = pl.ds(*slices[way])
        return pltpu.make_async_remote_copy(
            src_ref=parts[layer].at[flow, owner, span],
            dst_ref=gots[layer].at[flow, step, span],
            send_sem=ring_send.at[layer, flow, step, way],
            recv_sem=ring_recv.at[layer, flow, step, way],
            device_id={"slab": (ring_next, ring_prev)[way]},
            device_id_type=MESH,
        )

    def ring_owner(step, way):
        if way == 0:
            return slab_at((place + 2 * slabs - 1 - step) % slabs)
        return slab_at((place + 1 + step) % slabs)

    def ring_first(layer, flow):
        for way in range(2):
            ring_copy(layer, flow, 0, way, ring_owner(0, way)).start()

    def ring_event(layer, flow, step):
        for way in range(2):
            owner = ring_owner(step, way)
            span = pl.ds(*slices[way])
            ring_copy(layer, flow, step - 1, way, owner).wait_recv()
            value = parts[layer][flow, owner, span] + gots[layer][flow, step - 1, span]

            @pl.when(step < slabs - 1)
            def _():
                parts[layer][flow, owner, span] = value
                ring_copy(layer, flow, step, way, owner).start()

            @pl.when(step == slabs - 1)
            def _():
                outs[layer][(flow + 1) % 3, span] = value

    def ring_tick(layer, tick):
        flow = (tick + 1) % 3
        ahead = tick - 2 - 4 * flow
        step = (ahead + 30) // 3 - 10

        @pl.when((ahead >= 3) & (step <= slabs - 1))
        def _():
            ring_event(layer, flow, step)

    last_tick = 10 + 3 * (slabs - 1)

    def pack(layer, flow):
        lane = lax.broadcasted_iota(jnp.int32, (1, 128), 1) // block

        @pl.loop(0, rows // 72)
        def _(index):
            start = index * 72
            for tile in range(total // 128):
                pieces = [
                    raw[pl.ds(pl.multiple_of(v * rows + start, 8), 72), pl.ds(tile * 128, 128)]
                    for v in range(groups)
                ]
                for u in range(groups):
                    value = None
                    for v in range(groups):
                        piece = pieces[v]
                        if u != v:
                            piece = pltpu.roll(piece, ((v - u) * block) % 128, 1)
                        value = piece if value is None else jnp.where(lane == v, piece, value)
                    parts[layer][flow, tile * groups + u, pl.ds(pl.multiple_of(start, 8), 72)] = value

    def weight_chunk(layer, tick):
        flow, third_index = tick // 3, tick % 3
        depth = (flow + 1) % 3
        where = pl.ds(pl.multiple_of(third_index * third, third), third)
        window = lanes(2 - depth, planes)
        value = dot_nt(moved_h[where, :], full_h[:, window])
        value += dot_nt(moved_h[where, :], full_l[:, window])
        value += dot_nt(moved_l[where, :], full_h[:, window])
        raw[where, :] = value

        @pl.when(third_index == 2)
        def _():
            pack(layer, flow)
            ring_first(layer, flow)

    def conv_plane(plane):
        value = jnp.zeros((9 * channels, area), F32)
        for depth in range(3):
            window = lanes(plane + 2 - depth)
            value += dot_nn(taps_h[depth], full_h[:, window])
            value += dot_nn(taps_h[depth], full_l[:, window])
            value += dot_nn(taps_l[depth], full_h[:, window])
        mixed[...] = value

    def conv_sum(finish):
        @pl.loop(0, channels // 32)
        def _(index):
            start = pl.multiple_of(index * 32, 32)
            value = jnp.zeros((32, area), F32)
            for tap, (row_step, col_step) in enumerate(IN_PLANE):
                where = pl.ds(pl.multiple_of(tap * channels + start, 32), 32)
                value += shifted(mixed[where, :], -row_step, -col_step)
            finish(start, value)

    stage_copy(weight2_ref, 0).start()

    @pl.when(has_right)
    def _():
        rim_copy(0, 0, second_ref.at[:, lanes(planes - 1)]).start()

    @pl.when(has_left)
    def _():
        rim_copy(0, 1, second_ref.at[:, lanes(0)]).start()

    for slot in range(1, planes + 1):
        gather_start(0, slot, second_ref.at[:, lanes(slot - 1)])
    for slot in range(1, planes + 1):
        full[mine, lanes(slot)] = second_ref[:, lanes(slot - 1)]
    split_taps(weight2_ref)
    stage_copy(weight1_ref, 0).start()
    rim_gather(0)
    build_moved(hidden_ref)
    for slot in range(1, planes + 1):
        gather_forward(0, slot)
    rim_ends(0, functools.partial(gather_forward, 0))
    for slot in range(1, planes + 1):
        gather_finish(0, slot)
    rim_ends(0, functools.partial(gather_finish, 0))
    split_all()
    for slot in range(1, planes + 1):
        gather_sent(0, slot)
    rim_ends(0, functools.partial(gather_sent, 0))
    rim_sent(0)
    tell(free_sem)

    @pl.loop(0, 9)
    def _(tick):
        weight_chunk(0, tick)
        ring_tick(0, tick)

    pl.semaphore_wait(free_sem, chips + rims)

    @pl.loop(0, planes)
    def _(index):
        plane = (index + planes - 1) % planes
        conv_plane(plane)

        def finish(start, value):
            where = pl.ds(start, 32)
            target = pl.ds(pl.multiple_of(chan * channels + start, 32), 32)
            full[target, lanes(plane + 1)] = value * slope_ref[where, lanes(plane)]

        conv_sum(finish)
        view = full.at[mine, lanes(plane + 1)]

        @pl.when((plane == planes - 1) & has_right)
        def _():
            rim_copy(1, 0, view).start()

        @pl.when((plane == 0) & has_left)
        def _():
            rim_copy(1, 1, view).start()

        gather_start(1, plane + 1, view)

        @pl.when(index > 0)
        def _():
            gather_forward(1, (index + planes - 2) % planes + 1)

        @pl.when(index == 2)
        def _():
            rim_gather(1)

        @pl.when(index == planes - 1)
        def _():
            rim_ends(1, functools.partial(gather_forward, 1))

        ring_tick(0, index + 9)

    base = 9 + planes + 3
    build_moved(saved_ref)
    ring_tick(0, base - 3)
    gather_forward(1, planes - 1)
    split_taps(weight1_ref)
    ring_tick(0, base - 2)
    for slot in range(1, planes + 1):
        gather_finish(1, slot)
    rim_ends(1, functools.partial(gather_finish, 1))
    split_all()
    ring_tick(0, base - 1)

    @pl.loop(0, 9)
    def _(tick):
        weight_chunk(1, tick)
        ring_tick(0, base + tick)
        ring_tick(1, tick)

    @pl.loop(0, planes)
    def _(plane):
        conv_plane(plane)

        def finish(start, value):
            grad_ref[pl.ds(start, 32), lanes(plane)] = value

        conv_sum(finish)
        ring_tick(0, base + 9 + plane)
        ring_tick(1, 9 + plane)

    @pl.loop(9 + planes, last_tick + 1)
    def _(tick):
        ring_tick(0, base + tick)
        ring_tick(1, tick)

    for slot in range(1, planes + 1):
        gather_sent(1, slot)
    rim_ends(1, functools.partial(gather_sent, 1))
    rim_sent(1)
    for layer in range(2):
        for way in range(2):
            @pl.loop(0, 3)
            def _(flow):
                @pl.loop(0, slabs - 1)
                def _(step):
                    ring_copy(layer, flow, step, way, 0).wait_send()


def per_device(saved_input, pre_first, pre_second, out_grad, weight_first, weight_second):
    channels, planes, area = saved_input.shape
    total = weight_first.shape[2]
    slabs, chans = lax.axis_size("slab"), lax.axis_size("chan")
    side = math.isqrt(area)
    block = total // slabs
    groups = 128 // block
    rows = 9 * channels // groups
    width = planes * area
    flat = (channels, width)
    dims = (slabs, chans, total, planes, area, side)

    second_grad = (out_grad * silu_slope(pre_second)).reshape(flat)
    hidden = jax.nn.silu(pre_first).reshape(flat)
    slope = silu_slope(pre_first).reshape(flat)
    saved = saved_input.reshape(flat)
    wide = (planes + 2) * area
    chips = chans // 2
    vmem = pl.BlockSpec(memory_space=pltpu.VMEM)
    hbm = pl.BlockSpec(memory_space=pl.ANY)
    out_part = jax.ShapeDtypeStruct((3, rows, 128), F32)
    input_grad, first, second = pl.pallas_call(
        functools.partial(mega, dims),
        out_shape=(jax.ShapeDtypeStruct(flat, F32), out_part, out_part),
        in_specs=[vmem] * 4 + [hbm] * 2,
        out_specs=(vmem, vmem, vmem),
        scratch_shapes=[
            pltpu.VMEM((total, wide), F32),
            pltpu.VMEM((total, wide), BF16),
            pltpu.VMEM((total, wide), BF16),
            pltpu.VMEM((9 * channels, width), BF16),
            pltpu.VMEM((9 * channels, width), BF16),
            pltpu.VMEM((3, 9 * channels, total), BF16),
            pltpu.VMEM((3, 9 * channels, total), BF16),
            pltpu.VMEM((9 * channels, total), F32),
            pltpu.VMEM((9 * channels, total), F32),
            pltpu.VMEM((9 * channels, area), F32),
            pltpu.VMEM((3, slabs, rows, 128), F32),
            pltpu.VMEM((3, slabs, rows, 128), F32),
            pltpu.VMEM((3, slabs - 1, rows, 128), F32),
            pltpu.VMEM((3, slabs - 1, rows, 128), F32),
            pltpu.SemaphoreType.DMA((1,)),
            pltpu.SemaphoreType.DMA((2, planes + 2, 2 * chips)),
            pltpu.SemaphoreType.DMA((2, planes + 2, 2 * chips)),
            pltpu.SemaphoreType.DMA((2, 2)),
            pltpu.SemaphoreType.DMA((2, 2)),
            pltpu.SemaphoreType.DMA((2, 3, slabs - 1, 2)),
            pltpu.SemaphoreType.DMA((2, 3, slabs - 1, 2)),
            pltpu.SemaphoreType.REGULAR,
        ],
        compiler_params=pltpu.CompilerParams(
            collective_id=0, has_side_effects=True, vmem_limit_bytes=67043328
        ),
        name="backward",
    )(
        second_grad, hidden, saved, slope,
        weight_second.reshape(3, 9 * channels, total),
        weight_first.reshape(3, 9 * channels, total),
    )
    scale = math.sqrt(planes * slabs * area)

    def unpack(packed):
        value = packed.reshape(3, rows, groups, block).transpose(0, 2, 1, 3)
        return value.reshape(27, channels, block) / scale

    return input_grad.reshape(channels, planes, area), unpack(first), unpack(second)


def solution(mesh):
    in_specs = (
        P("chan", "slab", None),
        P("chan", "slab", None),
        P("chan", "slab", None),
        P("chan", "slab", None),
        P(None, "chan", None),
        P(None, "chan", None),
    )
    out_specs = (P("chan", "slab", None), P(None, "chan", "slab"), P(None, "chan", "slab"))
    return jax.shard_map(
        per_device, mesh=mesh, in_specs=in_specs, out_specs=out_specs, check_vma=False
    )
```

```python
import functools
import math

import jax
import jax.numpy as jnp
from jax import lax
from jax.experimental import pallas as pl
from jax.experimental.pallas import tpu as pltpu
from jax.sharding import PartitionSpec as P

F32 = jnp.float32
BF16 = jnp.bfloat16
MESH = pl.DeviceIdType.MESH
STEPS = (-1, 0, 1)
EVENTS = (
    ((1, 0, 2), (0, 1, 5)),
    ((1, 0, 3),),
    ((1, 1, 0),),
    ((1, 0, 4),),
    ((1, 1, 1),),
    ((1, 0, 5), (1, 1, 2)),
    ((1, 1, 3), (1, 1, 4), (1, 1, 5)),
)
IN_PLANE = [(row_step, col_step) for row_step in STEPS for col_step in STEPS]


def silu_slope(values):
    sigma = jax.nn.sigmoid(values)
    return sigma * (1.0 + values * (1.0 - sigma))


def halves(value):
    high = value.astype(BF16)
    return high, (value - high.astype(F32)).astype(BF16)


def dot_nn(left, right):
    return lax.dot_general(left, right, (((1,), (0,)), ((), ())), preferred_element_type=F32)


def dot_nt(left, right):
    return lax.dot_general(left, right, (((1,), (1,)), ((), ())), preferred_element_type=F32)


def mega(
    dims,
    saved_hbm, first_hbm, second_hbm, out_hbm, weight1_ref, weight2_ref,
    grad_ref, out1_ref, out2_ref,
    raw_second, raw_first, raw_out, sent, hidden, other2, other1,
    full, far, full_h, full_l, near_h, near_l, moved_h, moved_l, taps_h, taps_l,
    stage, raw, mixed, part2, part1, gotw2, gotw1, gotd2, gotd1, final,
    load_sem, stage_sem, gather_send, gather_recv, rim_send, rim_recv, pair_send, pair_recv,
    other_send, other_recv, wide_send, wide_recv, deep_send, deep_recv, store_sem, free_sem, slot_sem,
):
    slabs, chans, total, planes, area, side = dims
    channels = total // chans
    block = total // slabs
    groups = 128 // block
    rows = len(IN_PLANE) * channels // groups // 2
    chips = chans // 2
    members = slabs // 4
    owned = 2 * block
    half = total // 2
    width = planes * area
    wide = (planes + 2) * area
    steps = 9 * channels
    lump = steps // 2

    slab = lax.axis_index("slab")
    chan = lax.axis_index("chan")
    chip, core = chan // 2, chan % 2
    deep, across = slab // 2, slab % 2
    parity, member = deep % 2, deep // 2
    pair = slab + 2 - 4 * parity
    beside = slab + 1 - 2 * across
    partner = chip * 2 + 1 - core

    def kind_of(index):
        return (index * slabs // (2 * chans)) % 2

    takes = kind_of(chan) == parity
    gives = kind_of(chan) != parity

    def far_chan(j):
        return ((chip + j) % chips) * 2 + core

    def near_chan(j):
        return ((chip + chips - j) % chips) * 2 + core

    def crossed_chan(j):
        return ((chip + chips - j) % chips) * 2 + 1 - core

    def deep_slab(j):
        return 2 * (2 * ((member + j) % members) + parity) + across

    has_left = slab > 0
    has_right = slab < slabs - 1
    rims = jnp.minimum(slab, 1) + jnp.minimum(slabs - 1 - slab, 1)

    def signal(semaphore, **target):
        pl.semaphore_signal(semaphore, inc=1, device_id=target, device_id_type=MESH)

    def tell(semaphore):
        for j in range(1, chips):
            signal(semaphore, chan=far_chan(j))
        signal(semaphore, chan=partner)
        signal(semaphore, slab=pair)

        @pl.when(has_left)
        def _():
            signal(semaphore, slab=slab - 1)

        @pl.when(has_right)
        def _():
            signal(semaphore, slab=slab + 1)

    def load_copy(index):
        source = (second_hbm, out_hbm, first_hbm, saved_hbm)[index]
        target = (raw_second, raw_out, raw_first, raw_second)[index]
        return pltpu.make_async_copy(source, target, load_sem.at[index])

    def stage_copy(weight_ref, piece):
        source = weight_ref.at[piece // 2, pl.ds(piece % 2 * lump, lump)]
        return pltpu.make_async_copy(source, stage.at[piece % 2], stage_sem.at[piece % 2])

    for index in range(3):
        load_copy(index).start()
    stage_copy(weight2_ref, 0).start()
    stage_copy(weight2_ref, 1).start()

    barrier = pltpu.get_barrier_semaphore()
    tell(barrier)
    signal(barrier, slab=beside)
    for j in range(1, members):
        signal(barrier, slab=deep_slab(j))
    pl.semaphore_wait(barrier, 1 + members + chips + rims)

    def chan_rows(index):
        return pl.ds(pl.multiple_of(index * channels, channels), channels)

    def far_rows(index):
        start = index * channels
        group = start // (2 * owned)
        inside = start - (2 * group + kind_of(index)) * owned
        return pl.ds(pl.multiple_of(group * owned + inside, channels), channels)

    def lanes(slot, count=1):
        return pl.ds(pl.multiple_of(slot * area, area), count * area)

    mine = chan_rows(chan)

    def exists(kind, slot):
        base = (slab, pair)[kind]
        return (slot + base > 0) & (slot - (planes + 1) + base < slabs - 1)

    def rim_copy(layer, toward, source):
        return pltpu.make_async_remote_copy(
            src_ref=source,
            dst_ref=full.at[mine, lanes((0, planes + 1)[toward])],
            send_sem=rim_send.at[layer, toward],
            recv_sem=rim_recv.at[layer, toward],
            device_id={"slab": (slab + 1, slab - 1)[toward]},
            device_id_type=MESH,
        )

    def rim_start(layer):
        @pl.when(has_right)
        def _():
            rim_copy(layer, 0, sent.at[:, lanes(planes - 1)]).start()

        @pl.when(has_left)
        def _():
            rim_copy(layer, 1, sent.at[:, lanes(0)]).start()

    def rim_sent(layer):
        @pl.when(has_right)
        def _():
            rim_copy(layer, 0, sent.at[:, lanes(0)]).wait_send()

        @pl.when(has_left)
        def _():
            rim_copy(layer, 1, sent.at[:, lanes(0)]).wait_send()

    def pair_copy(layer, slot, source):
        return pltpu.make_async_remote_copy(
            src_ref=source,
            dst_ref=far.at[far_rows(chan), lanes(slot)],
            send_sem=pair_send.at[layer, slot],
            recv_sem=pair_recv.at[layer, slot],
            device_id={"slab": pair},
            device_id_type=MESH,
        )

    def other_copy(layer):
        return pltpu.make_async_remote_copy(
            src_ref=hidden,
            dst_ref=(other2, other1)[layer],
            send_sem=other_send.at[layer],
            recv_sem=other_recv.at[layer],
            device_id={"slab": pair},
            device_id_type=MESH,
        )

    def gather_copy(layer, kind, slot, source, owner, index, target):
        where = (chan_rows, far_rows)[kind](owner)
        return pltpu.make_async_remote_copy(
            src_ref=source,
            dst_ref=(full, far)[kind].at[where, lanes(slot)],
            send_sem=gather_send.at[layer, kind, slot, index],
            recv_sem=gather_recv.at[layer, kind, slot, index],
            device_id={"chan": target},
            device_id_type=MESH,
        )

    def held(kind, owner, slot):
        if kind == 0:
            return full.at[chan_rows(owner), lanes(slot)]
        return far.at[far_rows(owner), lanes(slot)]

    def guard(kind, owner):
        if kind == 0:
            return lambda action: action()
        return pl.when(kind_of(owner) == parity)

    def gather_start(layer, kind, slot, source):
        for j in range(1, chips):
            gather_copy(layer, kind, slot, source, chan, j, far_chan(j)).start()
        gather_copy(layer, kind, slot, source, chan, 0, partner).start()

    def gather_forward(layer, kind, slot):
        for j in range(1, chips):
            owner = near_chan(j)

            @guard(kind, owner)
            def _():
                view = held(kind, owner, slot)
                gather_copy(layer, kind, slot, view, owner, j, partner).wait_recv()
                gather_copy(layer, kind, slot, view, owner, chips + j, partner).start()

    def gather_finish(layer, kind, slot):
        @guard(kind, partner)
        def _():
            gather_copy(layer, kind, slot, held(kind, partner, slot), partner, 0, partner).wait_recv()

        for j in range(1, chips):
            owner = crossed_chan(j)

            @guard(kind, owner)
            def _():
                view = held(kind, owner, slot)
                gather_copy(layer, kind, slot, view, owner, chips + j, partner).wait_recv()

    def gather_sent(layer, kind, slot):
        @guard(kind, chan)
        def _():
            for index in range(chips):
                view = held(kind, chan, slot)
                gather_copy(layer, kind, slot, view, chan, index, partner).wait_send()

        for j in range(1, chips):
            owner = near_chan(j)

            @guard(kind, owner)
            def _():
                view = held(kind, owner, slot)
                gather_copy(layer, kind, slot, view, owner, chips + j, partner).wait_send()

    def slots_loop(action):
        @pl.loop(0, planes + 2)
        def _(index):
            action((index + 1) % (planes + 2))

    def when_exists(action, layer, kind):
        def run(slot):
            @pl.when(exists(kind, slot))
            def _():
                action(layer, kind, slot)

        return run

    def send_slot(layer, slot):
        gather_start(layer, 0, slot, sent.at[:, lanes(slot - 1)])

    def send_pair(layer, slot):
        @pl.when(gives)
        def _():
            pair_copy(layer, slot, sent.at[:, lanes(slot - 1)]).start()

    def rim_spread(layer):
        for toward in range(2):
            slot = (0, planes + 1)[toward]

            @pl.when((has_left, has_right)[toward])
            def _():
                view = full.at[mine, lanes(slot)]
                rim_copy(layer, toward, view).wait_recv()
                gather_start(layer, 0, slot, view)

                @pl.when(gives)
                def _():
                    pair_copy(layer, slot, view).start()

    def far_start(layer, kind, slot):
        @pl.when(takes)
        def _():
            view = held(1, chan, slot)
            pair_copy(layer, slot, view).wait_recv()
            gather_start(layer, 1, slot, view)

    def pair_sent(layer, slot):
        @pl.when(gives)
        def _():
            pair_copy(layer, slot, sent.at[:, lanes(0)]).wait_send()

    def slot_sent(layer, kind, slot):
        gather_sent(layer, 0, slot)
        pair_sent(layer, slot)

    def split_rows(source, start, high_ref, low_ref, target, slot):
        high, low = halves(source[pl.ds(start, 32), lanes(slot)])
        high_ref[pl.ds(target, 32), lanes(slot)] = high
        low_ref[pl.ds(target, 32), lanes(slot)] = low

    def split_full(slot):
        @pl.when(exists(0, slot))
        def _():
            @pl.loop(0, total // 32)
            def _(index):
                start = pl.multiple_of(index * 32, 32)
                split_rows(full, start, full_h, full_l, start, slot)

        @pl.when(jnp.logical_not(exists(0, slot)))
        def _():
            @pl.loop(0, total // 32)
            def _(index):
                where = pl.ds(pl.multiple_of(index * 32, 32), 32)
                full_h[where, lanes(slot)] = jnp.zeros((32, area), BF16)
                full_l[where, lanes(slot)] = jnp.zeros((32, area), BF16)

    def copy_near():
        @pl.loop(0, half // 32)
        def _(index):
            start = pl.multiple_of(index * 32, 32)
            group = start // owned
            where = pl.ds(pl.multiple_of(start + (group + parity) * owned, 32), 32)
            near_h[0, pl.ds(start, 32), :] = full_h[where, :]
            near_l[0, pl.ds(start, 32), :] = full_l[where, :]

    def split_far(slot):
        @pl.when(exists(1, slot))
        def _():
            @pl.loop(0, half // 32)
            def _(index):
                start = pl.multiple_of(index * 32, 32)
                split_rows(far, start, near_h.at[1], near_l.at[1], start, slot)

        @pl.when(jnp.logical_not(exists(1, slot)))
        def _():
            @pl.loop(0, half // 32)
            def _(index):
                where = pl.ds(pl.multiple_of(index * 32, 32), 32)
                near_h[1, where, lanes(slot)] = jnp.zeros((32, area), BF16)
                near_l[1, where, lanes(slot)] = jnp.zeros((32, area), BF16)

    cells = lax.broadcasted_iota(jnp.int32, (1, area), 1)
    row_ids, col_ids = cells // side, cells % side

    def mask_of(row_step, col_step):
        valid = (
            (row_ids + row_step >= 0)
            & (row_ids + row_step < side)
            & (col_ids + col_step >= 0)
            & (col_ids + col_step < side)
        )
        return jnp.where(valid, 1.0, 0.0).astype(F32)

    def shifted(value, row_step, col_step):
        if row_step == 0 and col_step == 0:
            return value
        shift = (-(row_step * side + col_step)) % area
        return pltpu.roll(value, shift, 1) * mask_of(row_step, col_step)

    def build_moved(piece, source):
        @pl.loop(0, planes)
        def _(plane):
            @pl.loop(0, channels // 32)
            def _(index):
                start = pl.multiple_of(index * 32, 32)
                value = source[pl.ds(start, 32), lanes(plane)]
                for tap, (row_step, col_step) in enumerate(IN_PLANE):
                    high, low = halves(shifted(value, row_step, col_step))
                    where = pl.ds(pl.multiple_of(tap * channels + start, 32), 32)
                    moved_h[piece, where, lanes(plane)] = high
                    moved_l[piece, where, lanes(plane)] = low

    def split_taps(weight_ref):
        for piece in range(6):
            stage_copy(weight_ref, piece).wait()

            @pl.loop(0, lump // 48)
            def _(index):
                start = pl.multiple_of(index * 48, 48)
                high, low = halves(stage[piece % 2, pl.ds(start, 48), :])
                where = pl.ds(pl.multiple_of(piece % 2 * lump + start, 48), 48)
                taps_h[piece // 2, where, :] = high
                taps_l[piece // 2, where, :] = low

            if piece < 4:
                stage_copy(weight_ref, piece + 2).start()

    parts, gotw, gotd = (part2, part1), (gotw2, gotw1), (gotd2, gotd1)
    outs = (out2_ref, out1_ref)

    def wide_copy(layer, flow):
        return pltpu.make_async_remote_copy(
            src_ref=parts[layer].at[flow, 1 - across],
            dst_ref=gotw[layer].at[flow],
            send_sem=wide_send.at[layer, flow],
            recv_sem=wide_recv.at[layer, flow],
            device_id={"slab": beside},
            device_id_type=MESH,
        )

    def deep_copy(layer, flow, j):
        return pltpu.make_async_remote_copy(
            src_ref=parts[layer].at[flow, across, (member + j) % members],
            dst_ref=gotd[layer].at[flow, j - 1],
            send_sem=deep_send.at[layer, flow, j - 1],
            recv_sem=deep_recv.at[layer, flow, j - 1],
            device_id={"slab": deep_slab(j)},
            device_id_type=MESH,
        )

    def store_copy(layer, flow):
        depth, where = (flow // 2 + 1) % 3, pl.ds(flow % 2 * lump, lump)
        return pltpu.make_async_copy(
            final.at[flow], outs[layer].at[depth, where], store_sem.at[layer, flow]
        )

    def rows_loop(action):
        if rows % 72:
            action(0, rows)
        else:

            @pl.loop(0, rows // 72)
            def _(part):
                action(pl.multiple_of(part * 72, 8), 72)

    def wide_event(layer, flow):
        wide_copy(layer, flow).wait_recv()
        for j in [*range(1, members), 0]:
            index = (member + j) % members

            def add(start, count):
                where = pl.ds(start, count)
                parts[layer][flow, across, index, where] = (
                    parts[layer][flow, across, index, where] + gotw[layer][flow, index, where]
                )

            rows_loop(add)
            if j:
                deep_copy(layer, flow, j).start()

    def deep_event(layer, flow):
        for j in range(1, members):
            deep_copy(layer, flow, j).wait_recv()
        if layer:
            store_copy(0, flow).wait()

        def add(start, count):
            where = pl.ds(start, count)
            value = parts[layer][flow, across, member, where]
            for j in range(1, members):
                value += gotd[layer][flow, j - 1, where]
            for v in range(groups):
                piece = pltpu.roll(value, (128 - v * block) % 128, 1) if v else value
                final[flow, pl.ds(v * rows + start, count), :] = piece[:, :block]

        rows_loop(add)
        store_copy(layer, flow).start()

    def pack(layer, flow):
        lane = lax.broadcasted_iota(jnp.int32, (1, 128), 1) // block

        def move(start, count):
            for tile in range(half // 128):
                pieces = [
                    raw[pl.ds(v * rows + start, count), pl.ds(tile * 128, 128)]
                    for v in range(groups)
                ]
                for u in range(groups):
                    value = None
                    for v in range(groups):
                        piece = pieces[v]
                        if u != v:
                            piece = pltpu.roll(piece, ((v - u) * block) % 128, 1)
                        value = piece if value is None else jnp.where(lane == v, piece, value)
                    owner = tile * groups + u
                    parts[layer][flow, owner % 2, owner // 2, pl.ds(start, count)] = value

        rows_loop(move)

    def weight_part(layer, flow):
        depth = (flow // 2 + 1) % 3
        window = lanes(2 - depth, planes)
        where = pl.ds(pl.multiple_of(flow % 2 * lump, lump), lump)
        value = jnp.zeros((lump, half), F32)
        for piece in range(2):
            value += dot_nt(moved_h[piece, where, :], near_h[piece, :, window])
            value += dot_nt(moved_h[piece, where, :], near_l[piece, :, window])
            value += dot_nt(moved_l[piece, where, :], near_h[piece, :, window])
        raw[...] = value
        pack(layer, flow)
        wide_copy(layer, flow).start()

    def conv_plane(plane):
        value = jnp.zeros((steps, area), F32)
        for depth in range(3):
            window = lanes(plane + 2 - depth)
            value += dot_nn(taps_h[depth], full_h[:, window])
            value += dot_nn(taps_h[depth], full_l[:, window])
            value += dot_nn(taps_l[depth], full_h[:, window])
        mixed[...] = value

    def conv_sum(finish):
        @pl.loop(0, channels // 32)
        def _(index):
            start = pl.multiple_of(index * 32, 32)
            value = jnp.zeros((32, area), F32)
            for tap, (row_step, col_step) in enumerate(IN_PLANE):
                where = pl.ds(pl.multiple_of(tap * channels + start, 32), 32)
                value += shifted(mixed[where, :], -row_step, -col_step)
            finish(start, value)

    def each_plane(action):
        @pl.loop(0, planes)
        def _(plane):
            @pl.loop(0, channels // 32)
            def _(index):
                action(plane, pl.ds(pl.multiple_of(index * 32, 32), 32))

    load_copy(0).wait()
    load_copy(1).wait()

    def make_sent(plane, where):
        sent[where, lanes(plane)] = raw_out[plane, where, :] * silu_slope(raw_second[plane, where, :])

    each_plane(make_sent)
    rim_start(0)
    for slot in range(1, 4):
        send_slot(0, slot)
    for slot in range(1, planes + 1):
        send_pair(0, slot)
    load_copy(3).start()
    load_copy(2).wait()

    def make_hidden(plane, where):
        value = raw_first[plane, where, :]
        hidden[where, lanes(plane)] = value * jax.nn.sigmoid(value)

    each_plane(make_hidden)

    def keep_sent(plane, where):
        target = pl.ds(pl.multiple_of(chan * channels + where.start, 32), 32)
        full[target, lanes(plane + 1)] = sent[where, lanes(plane)]

    each_plane(keep_sent)
    split_taps(weight2_ref)
    stage_copy(weight1_ref, 0).start()
    stage_copy(weight1_ref, 1).start()
    for slot in range(4, planes + 1):
        send_slot(0, slot)
    rim_spread(0)
    build_moved(0, hidden)
    other_copy(0).start()
    for slot in (1, 2):
        gather_forward(0, 0, slot)
    gather_forward(0, 0, 3)
    for slot in (1, 2):
        gather_finish(0, 0, slot)
        split_full(slot)

    def when_far(action, layer):
        return when_exists(action, layer, 1)

    def make_saved(plane, where):
        hidden[where, lanes(plane)] = raw_second[plane, where, :]

    @pl.loop(0, planes)
    def _(index):
        plane = (index + 1) % planes
        slot = (index + 3) % (planes + 2)

        @pl.when(exists(0, slot))
        def _():
            gather_finish(0, 0, slot)

        split_full(slot)
        slot_sent(0, 0, plane + 1)
        for j in range(1, chips):
            signal(slot_sem.at[plane], chan=far_chan(j))
        signal(slot_sem.at[plane], chan=partner)
        conv_plane(plane)
        following = (index + 4) % (planes + 2)

        @pl.when((index < planes - 1) & exists(0, following))
        def _():
            gather_forward(0, 0, following)

        @pl.when(index == 0)
        def _():
            for late in range(1, planes + 1):
                far_start(0, 1, late)
            for late in (planes + 1, 0):
                when_far(far_start, 0)(late)

        @pl.when(index == planes - 2)
        def _():
            load_copy(3).wait()
            other_copy(0).wait_send()
            each_plane(make_saved)
            other_copy(1).start()

        @pl.when((plane == 0) & has_left)
        def _():
            rim_copy(0, 1, sent.at[:, lanes(0)]).wait_send()

        @pl.when((plane == planes - 1) & has_right)
        def _():
            rim_copy(0, 0, sent.at[:, lanes(0)]).wait_send()

        def finish(start, value):
            where = pl.ds(start, 32)
            target = pl.ds(pl.multiple_of(chan * channels + start, 32), 32)
            value = value * silu_slope(raw_first[plane, where, :])
            sent[where, lanes(plane)] = value
            full[target, lanes(plane + 1)] = value

        conv_sum(finish)
        pl.semaphore_wait(slot_sem.at[plane], chips)
        send_slot(1, plane + 1)

    other_copy(0).wait_recv()
    build_moved(1, other2)
    copy_near()
    slots_loop(when_far(gather_forward, 0))
    slots_loop(when_far(gather_finish, 0))
    slots_loop(split_far)
    for slot in (planes + 1, 0):
        when_exists(slot_sent, 0, 0)(slot)
    slots_loop(when_far(gather_sent, 0))
    tell(free_sem)

    @pl.loop(0, 6)
    def _(flow):
        weight_part(0, flow)

        @pl.when(flow == 0)
        def _():
            pl.semaphore_wait(free_sem, 1 + chips + rims)
            rim_start(1)
            for slot in range(1, planes + 1):
                send_pair(1, slot)

        @pl.when(flow == 2)
        def _():
            rim_spread(1)
            for slot in range(2, 4):
                gather_forward(1, 0, slot)

        @pl.when(flow == 3)
        def _():
            wide_event(0, 0)

        @pl.when(flow == 4)
        def _():
            for slot in range(1, planes + 1):
                far_start(1, 1, slot)
            for slot in (planes + 1, 0):
                when_far(far_start, 1)(slot)

    wide_event(0, 1)
    for slot in (*range(4, planes + 1), 1):
        gather_forward(1, 0, slot)
    build_moved(0, hidden)
    other_copy(1).wait_recv()
    wide_event(0, 2)
    build_moved(1, other1)
    for slot in (planes + 1, 0):
        when_exists(gather_forward, 1, 0)(slot)
    slots_loop(when_far(gather_forward, 1))
    slots_loop(when_exists(gather_finish, 1, 0))
    slots_loop(split_full)
    copy_near()
    slots_loop(when_far(gather_finish, 1))
    slots_loop(split_far)
    wide_event(0, 3)

    @pl.loop(0, 6)
    def _(flow):
        weight_part(1, flow)

        @pl.when((flow == 1) | (flow == 3))
        def _():
            wide_event(0, 4 + flow // 2)

        @pl.when(flow == 4)
        def _():
            wide_event(1, 0)

    split_taps(weight1_ref)
    wide_event(1, 1)
    for flow in range(5):
        deep_event(0, flow)

    @pl.loop(0, planes)
    def _(plane):
        conv_plane(plane)

        def finish(start, value):
            raw_out[plane, pl.ds(start, 32), :] = value

        conv_sum(finish)
        for index in range(min(planes, 6)):
            @pl.when(plane == index)
            def _():
                for layer, kind, flow in EVENTS[index]:
                    (wide_event, deep_event)[kind](layer, flow)

    result = pltpu.make_async_copy(raw_out, grad_ref, load_sem.at[0])
    result.start()
    for late in [*EVENTS[min(planes, 6) : 6], EVENTS[6]]:
        for layer, kind, flow in late:
            (wide_event, deep_event)[kind](layer, flow)
    result.wait()
    for flow in range(6):
        store_copy(1, flow).wait()
    slots_loop(when_exists(slot_sent, 1, 0))
    slots_loop(when_far(gather_sent, 1))
    rim_sent(1)
    other_copy(1).wait_send()
    for layer in range(2):
        for flow in range(6):
            wide_copy(layer, flow).wait_send()
            for j in range(1, members):
                deep_copy(layer, flow, j).wait_send()


def per_device(saved_input, pre_first, pre_second, out_grad, weight_first, weight_second):
    channels, planes, area = saved_input.shape
    total = weight_first.shape[2]
    slabs, chans = lax.axis_size("slab"), lax.axis_size("chan")
    side = math.isqrt(area)
    block = total // slabs
    groups = 128 // block
    steps = 9 * channels
    rows = steps // groups // 2
    width = planes * area
    wide = (planes + 2) * area
    chips, members, half = chans // 2, slabs // 4, total // 2
    dims = (slabs, chans, total, planes, area, side)
    hbm = pl.BlockSpec(memory_space=pl.ANY)
    cube = pltpu.VMEM((planes, channels, area), F32)
    flat = pltpu.VMEM((channels, width), F32)
    dma = pltpu.SemaphoreType.DMA
    out_part = jax.ShapeDtypeStruct((3, steps, block), F32)
    input_grad, first, second = pl.pallas_call(
        functools.partial(mega, dims),
        out_shape=(jax.ShapeDtypeStruct((planes, channels, area), F32), out_part, out_part),
        in_specs=[hbm] * 6,
        out_specs=(hbm, hbm, hbm),
        scratch_shapes=[
            *[cube] * 3,
            *[flat] * 4,
            pltpu.VMEM((total, wide), F32),
            pltpu.VMEM((half, wide), F32),
            *[pltpu.VMEM((total, wide), BF16)] * 2,
            *[pltpu.VMEM((2, half, wide), BF16)] * 2,
            *[pltpu.VMEM((2, steps, width), BF16)] * 2,
            *[pltpu.VMEM((3, steps, total), BF16)] * 2,
            pltpu.VMEM((2, steps // 2, total), F32),
            pltpu.VMEM((steps // 2, half), F32),
            pltpu.VMEM((steps, area), F32),
            *[pltpu.VMEM((6, 2, members, rows, 128), F32)] * 2,
            *[pltpu.VMEM((6, members, rows, 128), F32)] * 2,
            *[pltpu.VMEM((6, max(members - 1, 1), rows, 128), F32)] * 2,
            pltpu.VMEM((6, steps // 2, block), F32),
            dma((4,)),
            dma((2,)),
            *[dma((2, 2, planes + 2, 2 * chips))] * 2,
            *[dma((2, 2))] * 2,
            *[dma((2, planes + 2))] * 2,
            *[dma((2,))] * 2,
            *[dma((2, 6))] * 2,
            *[dma((2, 6, max(members - 1, 1)))] * 2,
            dma((2, 6)),
            pltpu.SemaphoreType.REGULAR,
            pltpu.SemaphoreType.REGULAR((planes,)),
        ],
        compiler_params=pltpu.CompilerParams(
            collective_id=0, has_side_effects=True, vmem_limit_bytes=67043328
        ),
        name="backward",
    )(
        *(value.transpose(1, 0, 2) for value in (saved_input, pre_first, pre_second, out_grad)),
        weight_first.reshape(3, steps, total),
        weight_second.reshape(3, steps, total),
    )
    scale = math.sqrt(planes * slabs * area)

    def finish(packed):
        return packed.reshape(27, channels, block) / scale

    return input_grad.transpose(1, 0, 2), finish(first), finish(second)


def solution(mesh):
    in_specs = (
        P("chan", "slab", None),
        P("chan", "slab", None),
        P("chan", "slab", None),
        P("chan", "slab", None),
        P(None, "chan", None),
        P(None, "chan", None),
    )
    out_specs = (P("chan", "slab", None), P(None, "chan", "slab"), P(None, "chan", "slab"))
    return jax.shard_map(
        per_device, mesh=mesh, in_specs=in_specs, out_specs=out_specs, check_vma=False
    )
```

```python
import functools
import math

import jax
import jax.numpy as jnp
from jax import lax
from jax.experimental import pallas as pl
from jax.experimental.pallas import tpu as pltpu
from jax.sharding import PartitionSpec as P

F32 = jnp.float32
BF16 = jnp.bfloat16
MESH = pl.DeviceIdType.MESH
STEPS = (-1, 0, 1)
EVENTS = (
    ((1, 0, 3), (0, 1, 5)),
    ((1, 1, 0),),
    ((1, 0, 4), (1, 1, 1)),
    ((1, 0, 5),),
    ((1, 1, 2),),
    ((1, 1, 3),),
    ((1, 1, 4), (1, 1, 5)),
)
IN_PLANE = [(row_step, col_step) for row_step in STEPS for col_step in STEPS]


def silu_slope(values):
    sigma = jax.nn.sigmoid(values)
    return sigma * (1.0 + values * (1.0 - sigma))


def halves(value):
    high = value.astype(BF16)
    return high, (value - high.astype(F32)).astype(BF16)


def dot_nn(left, right):
    return lax.dot_general(left, right, (((1,), (0,)), ((), ())), preferred_element_type=F32)


def dot_nt(left, right):
    return lax.dot_general(left, right, (((1,), (1,)), ((), ())), preferred_element_type=F32)


def mega(
    dims,
    saved_hbm, first_hbm, second_hbm, out_hbm, weight1_ref, weight2_ref,
    grad_ref, out1_ref, out2_ref,
    raw_second, raw_first, raw_out, sent, hidden, other2, other1,
    full, far, full_h, full_l, near_h, near_l, moved_h, moved_l, taps_h, taps_l,
    stage, raw, mixed, part2, part1, gotw2, gotw1, gotd2, gotd1, final,
    load_sem, stage_sem, gather_send, gather_recv, rim_send, rim_recv, pair_send, pair_recv,
    other_send, other_recv, wide_send, wide_recv, deep_send, deep_recv, store_sem, free_sem, slot_sem,
):
    slabs, chans, total, planes, area, side = dims
    channels = total // chans
    block = total // slabs
    groups = 128 // block
    rows = len(IN_PLANE) * channels // groups // 2
    chips = chans // 2
    members = slabs // 4
    owned = 2 * block
    half = total // 2
    width = planes * area
    wide = (planes + 2) * area
    steps = 9 * channels
    lump = steps // 2

    slab = lax.axis_index("slab")
    chan = lax.axis_index("chan")
    chip, core = chan // 2, chan % 2
    deep, across = slab // 2, slab % 2
    parity, member = deep % 2, deep // 2
    pair = slab + 2 - 4 * parity
    beside = slab + 1 - 2 * across
    partner = chip * 2 + 1 - core

    def kind_of(index):
        return (index * slabs // (2 * chans)) % 2

    takes = kind_of(chan) == parity
    gives = kind_of(chan) != parity

    def far_chan(j):
        return ((chip + j) % chips) * 2 + core

    def near_chan(j):
        return ((chip + chips - j) % chips) * 2 + core

    def crossed_chan(j):
        return ((chip + chips - j) % chips) * 2 + 1 - core

    def deep_slab(j):
        return 2 * (2 * ((member + j) % members) + parity) + across

    has_left = slab > 0
    has_right = slab < slabs - 1
    rims = jnp.minimum(slab, 1) + jnp.minimum(slabs - 1 - slab, 1)

    def signal(semaphore, **target):
        pl.semaphore_signal(semaphore, inc=1, device_id=target, device_id_type=MESH)

    def tell(semaphore):
        for j in range(1, chips):
            signal(semaphore, chan=far_chan(j))
        signal(semaphore, chan=partner)
        signal(semaphore, slab=pair)

        @pl.when(has_left)
        def _():
            signal(semaphore, slab=slab - 1)

        @pl.when(has_right)
        def _():
            signal(semaphore, slab=slab + 1)

    def load_copy(index):
        source = (second_hbm, out_hbm, first_hbm, saved_hbm)[index]
        target = (raw_second, raw_out, raw_first, raw_second)[index]
        return pltpu.make_async_copy(source, target, load_sem.at[index])

    def stage_copy(weight_ref, piece):
        source = weight_ref.at[piece // 2, pl.ds(piece % 2 * lump, lump)]
        return pltpu.make_async_copy(source, stage.at[piece % 2], stage_sem.at[piece % 2])

    for index in range(3):
        load_copy(index).start()
    stage_copy(weight2_ref, 0).start()
    stage_copy(weight2_ref, 1).start()

    barrier = pltpu.get_barrier_semaphore()
    tell(barrier)
    signal(barrier, slab=beside)
    for j in range(1, members):
        signal(barrier, slab=deep_slab(j))

    def chan_rows(index):
        return pl.ds(pl.multiple_of(index * channels, channels), channels)

    def far_rows(index):
        start = index * channels
        group = start // (2 * owned)
        inside = start - (2 * group + kind_of(index)) * owned
        return pl.ds(pl.multiple_of(group * owned + inside, channels), channels)

    def lanes(slot, count=1):
        return pl.ds(pl.multiple_of(slot * area, area), count * area)

    mine = chan_rows(chan)

    def exists(kind, slot):
        base = (slab, pair)[kind]
        return (slot + base > 0) & (slot - (planes + 1) + base < slabs - 1)

    def rim_copy(layer, toward, source):
        return pltpu.make_async_remote_copy(
            src_ref=source,
            dst_ref=full.at[mine, lanes((0, planes + 1)[toward])],
            send_sem=rim_send.at[layer, toward],
            recv_sem=rim_recv.at[layer, toward],
            device_id={"slab": (slab + 1, slab - 1)[toward]},
            device_id_type=MESH,
        )

    def rim_start(layer):
        @pl.when(has_right)
        def _():
            rim_copy(layer, 0, sent.at[:, lanes(planes - 1)]).start()

        @pl.when(has_left)
        def _():
            rim_copy(layer, 1, sent.at[:, lanes(0)]).start()

    def rim_sent(layer):
        @pl.when(has_right)
        def _():
            rim_copy(layer, 0, sent.at[:, lanes(0)]).wait_send()

        @pl.when(has_left)
        def _():
            rim_copy(layer, 1, sent.at[:, lanes(0)]).wait_send()

    def pair_copy(layer, slot, source):
        return pltpu.make_async_remote_copy(
            src_ref=source,
            dst_ref=far.at[far_rows(chan), lanes(slot)],
            send_sem=pair_send.at[layer, slot],
            recv_sem=pair_recv.at[layer, slot],
            device_id={"slab": pair},
            device_id_type=MESH,
        )

    def other_copy(layer):
        return pltpu.make_async_remote_copy(
            src_ref=(hidden, raw_second)[layer],
            dst_ref=(other2, other1)[layer],
            send_sem=other_send.at[layer],
            recv_sem=other_recv.at[layer],
            device_id={"slab": pair},
            device_id_type=MESH,
        )

    def gather_copy(layer, kind, slot, source, owner, index, target):
        where = (chan_rows, far_rows)[kind](owner)
        return pltpu.make_async_remote_copy(
            src_ref=source,
            dst_ref=(full, far)[kind].at[where, lanes(slot)],
            send_sem=gather_send.at[layer, kind, slot, index],
            recv_sem=gather_recv.at[layer, kind, slot, index],
            device_id={"chan": target},
            device_id_type=MESH,
        )

    def held(kind, owner, slot):
        if kind == 0:
            return full.at[chan_rows(owner), lanes(slot)]
        return far.at[far_rows(owner), lanes(slot)]

    def guard(kind, owner):
        if kind == 0:
            return lambda action: action()
        return pl.when(kind_of(owner) == parity)

    def gather_start(layer, kind, slot, source):
        for j in range(1, chips):
            gather_copy(layer, kind, slot, source, chan, j, far_chan(j)).start()
        gather_copy(layer, kind, slot, source, chan, 0, partner).start()

    def gather_forward(layer, kind, slot):
        for j in range(1, chips):
            owner = near_chan(j)

            @guard(kind, owner)
            def _():
                view = held(kind, owner, slot)
                gather_copy(layer, kind, slot, view, owner, j, partner).wait_recv()
                gather_copy(layer, kind, slot, view, owner, chips + j, partner).start()

    def gather_finish(layer, kind, slot):
        @guard(kind, partner)
        def _():
            gather_copy(layer, kind, slot, held(kind, partner, slot), partner, 0, partner).wait_recv()

        for j in range(1, chips):
            owner = crossed_chan(j)

            @guard(kind, owner)
            def _():
                view = held(kind, owner, slot)
                gather_copy(layer, kind, slot, view, owner, chips + j, partner).wait_recv()

    def gather_sent(layer, kind, slot):
        @guard(kind, chan)
        def _():
            for index in range(chips):
                view = held(kind, chan, slot)
                gather_copy(layer, kind, slot, view, chan, index, partner).wait_send()

        for j in range(1, chips):
            owner = near_chan(j)

            @guard(kind, owner)
            def _():
                view = held(kind, owner, slot)
                gather_copy(layer, kind, slot, view, owner, chips + j, partner).wait_send()

    def slots_loop(action):
        @pl.loop(0, planes + 2)
        def _(index):
            action((index + 1) % (planes + 2))

    def when_exists(action, layer, kind):
        def run(slot):
            @pl.when(exists(kind, slot))
            def _():
                action(layer, kind, slot)

        return run

    def send_slot(layer, slot):
        gather_start(layer, 0, slot, sent.at[:, lanes(slot - 1)])

    def send_pair(layer, slot):
        @pl.when(gives)
        def _():
            pair_copy(layer, slot, sent.at[:, lanes(slot - 1)]).start()

    def rim_take(layer):
        for toward in range(2):
            slot = (0, planes + 1)[toward]

            @pl.when((has_left, has_right)[toward])
            def _():
                view = full.at[mine, lanes(slot)]
                rim_copy(layer, toward, view).wait_recv()

                @pl.when(gives)
                def _():
                    pair_copy(layer, slot, view).start()

    def rim_spread(layer):
        for slot in (planes + 1, 0):

            @pl.when(exists(0, slot))
            def _():
                gather_start(layer, 0, slot, full.at[mine, lanes(slot)])

    def far_start(layer, kind, slot):
        @pl.when(takes)
        def _():
            view = held(1, chan, slot)
            pair_copy(layer, slot, view).wait_recv()
            gather_start(layer, 1, slot, view)

    def pair_sent(layer, slot):
        @pl.when(gives)
        def _():
            pair_copy(layer, slot, sent.at[:, lanes(0)]).wait_send()

    def slot_sent(layer, kind, slot):
        gather_sent(layer, 0, slot)
        pair_sent(layer, slot)

    def split_rows(source, start, high_ref, low_ref, target, slot):
        high, low = halves(source[pl.ds(start, 32), lanes(slot)])
        high_ref[pl.ds(target, 32), lanes(slot)] = high
        low_ref[pl.ds(target, 32), lanes(slot)] = low

    def split_full(slot):
        @pl.when(exists(0, slot))
        def _():
            @pl.loop(0, total // 32)
            def _(index):
                start = pl.multiple_of(index * 32, 32)
                split_rows(full, start, full_h, full_l, start, slot)

        @pl.when(jnp.logical_not(exists(0, slot)))
        def _():
            @pl.loop(0, total // 32)
            def _(index):
                where = pl.ds(pl.multiple_of(index * 32, 32), 32)
                full_h[where, lanes(slot)] = jnp.zeros((32, area), BF16)
                full_l[where, lanes(slot)] = jnp.zeros((32, area), BF16)

    def copy_near(slot, count):
        @pl.loop(0, half // 32)
        def _(index):
            start = pl.multiple_of(index * 32, 32)
            group = start // owned
            where = pl.ds(pl.multiple_of(start + (group + parity) * owned, 32), 32)
            near_h[0, pl.ds(start, 32), lanes(slot, count)] = full_h[where, lanes(slot, count)]
            near_l[0, pl.ds(start, 32), lanes(slot, count)] = full_l[where, lanes(slot, count)]

    def split_far(slot):
        @pl.when(exists(1, slot))
        def _():
            @pl.loop(0, half // 32)
            def _(index):
                start = pl.multiple_of(index * 32, 32)
                split_rows(far, start, near_h.at[1], near_l.at[1], start, slot)

        @pl.when(jnp.logical_not(exists(1, slot)))
        def _():
            @pl.loop(0, half // 32)
            def _(index):
                where = pl.ds(pl.multiple_of(index * 32, 32), 32)
                near_h[1, where, lanes(slot)] = jnp.zeros((32, area), BF16)
                near_l[1, where, lanes(slot)] = jnp.zeros((32, area), BF16)

    cells = lax.broadcasted_iota(jnp.int32, (1, area), 1)
    row_ids, col_ids = cells // side, cells % side

    def mask_of(row_step, col_step):
        valid = (
            (row_ids + row_step >= 0)
            & (row_ids + row_step < side)
            & (col_ids + col_step >= 0)
            & (col_ids + col_step < side)
        )
        return jnp.where(valid, 1.0, 0.0).astype(F32)

    def shifted(value, row_step, col_step):
        if row_step == 0 and col_step == 0:
            return value
        shift = (-(row_step * side + col_step)) % area
        return pltpu.roll(value, shift, 1) * mask_of(row_step, col_step)

    def flat_rows(source):
        return lambda plane, where: source[where, lanes(plane)]

    def cube_rows(source):
        return lambda plane, where: source[plane, where, :]

    def build_moved(piece, source):
        @pl.loop(0, planes)
        def _(plane):
            @pl.loop(0, channels // 32)
            def _(index):
                start = pl.multiple_of(index * 32, 32)
                value = source(plane, pl.ds(start, 32))
                for tap, (row_step, col_step) in enumerate(IN_PLANE):
                    high, low = halves(shifted(value, row_step, col_step))
                    where = pl.ds(pl.multiple_of(tap * channels + start, 32), 32)
                    moved_h[piece, where, lanes(plane)] = high
                    moved_l[piece, where, lanes(plane)] = low

    def split_taps(weight_ref):
        for piece in range(6):
            stage_copy(weight_ref, piece).wait()

            @pl.loop(0, lump // 48)
            def _(index):
                start = pl.multiple_of(index * 48, 48)
                high, low = halves(stage[piece % 2, pl.ds(start, 48), :])
                where = pl.ds(pl.multiple_of(piece % 2 * lump + start, 48), 48)
                taps_h[piece // 2, where, :] = high
                taps_l[piece // 2, where, :] = low

            if piece < 4:
                stage_copy(weight_ref, piece + 2).start()

    parts, gotw, gotd = (part2, part1), (gotw2, gotw1), (gotd2, gotd1)
    outs = (out2_ref, out1_ref)

    def wide_copy(layer, flow):
        return pltpu.make_async_remote_copy(
            src_ref=parts[layer].at[flow, 1 - across],
            dst_ref=gotw[layer].at[flow],
            send_sem=wide_send.at[layer, flow],
            recv_sem=wide_recv.at[layer, flow],
            device_id={"slab": beside},
            device_id_type=MESH,
        )

    def deep_copy(layer, flow, j):
        return pltpu.make_async_remote_copy(
            src_ref=parts[layer].at[flow, across, (member + j) % members],
            dst_ref=gotd[layer].at[flow, j - 1],
            send_sem=deep_send.at[layer, flow, j - 1],
            recv_sem=deep_recv.at[layer, flow, j - 1],
            device_id={"slab": deep_slab(j)},
            device_id_type=MESH,
        )

    def store_copy(layer, flow):
        depth, where = (flow // 2 + 1) % 3, pl.ds(flow % 2 * lump, lump)
        return pltpu.make_async_copy(
            final.at[flow], outs[layer].at[depth, where], store_sem.at[layer, flow]
        )

    def rows_loop(action):
        if rows % 72:
            action(0, rows)
        else:

            @pl.loop(0, rows // 72)
            def _(part):
                action(pl.multiple_of(part * 72, 8), 72)

    def wide_event(layer, flow):
        wide_copy(layer, flow).wait_recv()
        for j in [*range(1, members), 0]:
            index = (member + j) % members

            def add(start, count):
                where = pl.ds(start, count)
                parts[layer][flow, across, index, where] = (
                    parts[layer][flow, across, index, where] + gotw[layer][flow, index, where]
                )

            rows_loop(add)
            if j:
                deep_copy(layer, flow, j).start()

    def deep_event(layer, flow):
        for j in range(1, members):
            deep_copy(layer, flow, j).wait_recv()
        if layer:
            store_copy(0, flow).wait()

        def add(start, count):
            where = pl.ds(start, count)
            value = parts[layer][flow, across, member, where]
            for j in range(1, members):
                value += gotd[layer][flow, j - 1, where]
            for v in range(groups):
                piece = pltpu.roll(value, (128 - v * block) % 128, 1) if v else value
                final[flow, pl.ds(v * rows + start, count), :] = piece[:, :block]

        rows_loop(add)
        store_copy(layer, flow).start()

    def pack(layer, flow):
        lane = lax.broadcasted_iota(jnp.int32, (1, 128), 1) // block

        def move(start, count):
            for tile in range(half // 128):
                pieces = [
                    raw[pl.ds(v * rows + start, count), pl.ds(tile * 128, 128)]
                    for v in range(groups)
                ]
                for u in range(groups):
                    value = None
                    for v in range(groups):
                        piece = pieces[v]
                        if u != v:
                            piece = pltpu.roll(piece, ((v - u) * block) % 128, 1)
                        value = piece if value is None else jnp.where(lane == v, piece, value)
                    owner = tile * groups + u
                    parts[layer][flow, owner % 2, owner // 2, pl.ds(start, count)] = value

        rows_loop(move)

    def weight_part(layer, flow):
        depth = (flow // 2 + 1) % 3
        window = lanes(2 - depth, planes)
        where = pl.ds(pl.multiple_of(flow % 2 * lump, lump), lump)
        value = jnp.zeros((lump, half), F32)
        for piece in range(2):
            value += dot_nt(moved_h[piece, where, :], near_h[piece, :, window])
            value += dot_nt(moved_h[piece, where, :], near_l[piece, :, window])
            value += dot_nt(moved_l[piece, where, :], near_h[piece, :, window])
        raw[...] = value
        pack(layer, flow)

    def conv_plane(plane):
        value = jnp.zeros((steps, area), F32)
        for depth in range(3):
            window = lanes(plane + 2 - depth)
            value += dot_nn(taps_h[depth], full_h[:, window])
            value += dot_nn(taps_h[depth], full_l[:, window])
            value += dot_nn(taps_l[depth], full_h[:, window])
        mixed[...] = value

    def conv_sum(finish):
        @pl.loop(0, channels // 32)
        def _(index):
            start = pl.multiple_of(index * 32, 32)
            value = jnp.zeros((32, area), F32)
            for tap, (row_step, col_step) in enumerate(IN_PLANE):
                where = pl.ds(pl.multiple_of(tap * channels + start, 32), 32)
                value += shifted(mixed[where, :], -row_step, -col_step)
            finish(start, value)

    def each_plane(action):
        @pl.loop(0, planes)
        def _(plane):
            @pl.loop(0, channels // 32)
            def _(index):
                action(plane, pl.ds(pl.multiple_of(index * 32, 32), 32))

    load_copy(0).wait()
    load_copy(1).wait()

    def make_sent(plane, where):
        sent[where, lanes(plane)] = raw_out[plane, where, :] * silu_slope(raw_second[plane, where, :])

    each_plane(make_sent)
    load_copy(3).start()
    load_copy(2).wait()

    def make_hidden(plane, where):
        value = raw_first[plane, where, :]
        hidden[where, lanes(plane)] = value * jax.nn.sigmoid(value)

    each_plane(make_hidden)
    pl.semaphore_wait(barrier, 1 + members + chips + rims)
    rim_start(0)
    for slot in range(1, 4):
        send_slot(0, slot)
    for slot in range(1, planes + 1):
        send_pair(0, slot)

    def keep_sent(plane, where):
        target = pl.ds(pl.multiple_of(chan * channels + where.start, 32), 32)
        full[target, lanes(plane + 1)] = sent[where, lanes(plane)]

    each_plane(keep_sent)
    split_taps(weight2_ref)
    stage_copy(weight1_ref, 0).start()
    stage_copy(weight1_ref, 1).start()
    for slot in range(4, planes + 1):
        send_slot(0, slot)
    rim_take(0)
    other_copy(0).start()
    build_moved(0, flat_rows(hidden))
    for slot in (1, 2, 3):
        gather_forward(0, 0, slot)
    for slot in (1, 2):
        gather_finish(0, 0, slot)
        split_full(slot)

    def when_far(action, layer):
        return when_exists(action, layer, 1)

    def inner_slots(action):
        @pl.loop(1, planes + 1)
        def _(slot):
            action(slot)

    def conv_step(plane):
        slot_sent(0, 0, plane + 1)
        for j in range(1, chips):
            signal(slot_sem.at[plane], chan=far_chan(j))
        signal(slot_sem.at[plane], chan=partner)
        conv_plane(plane)

    def conv_finish(plane):
        @pl.when((plane == 0) & has_left)
        def _():
            rim_copy(0, 1, sent.at[:, lanes(0)]).wait_send()

        @pl.when((plane == planes - 1) & has_right)
        def _():
            rim_copy(0, 0, sent.at[:, lanes(0)]).wait_send()

        def finish(start, value):
            where = pl.ds(start, 32)
            target = pl.ds(pl.multiple_of(chan * channels + start, 32), 32)
            value = value * silu_slope(raw_first[plane, where, :])
            sent[where, lanes(plane)] = value
            full[target, lanes(plane + 1)] = value

        conv_sum(finish)

    def send_result(plane):
        pl.semaphore_wait(slot_sem.at[plane], chips)
        send_slot(1, plane + 1)

    @pl.loop(0, planes - 2)
    def _(index):
        plane = index + 1
        slot = index + 3
        gather_finish(0, 0, slot)
        split_full(slot)
        conv_step(plane)

        @pl.when(index < planes - 3)
        def _():
            gather_forward(0, 0, slot + 1)

        @pl.when(index == 0)
        def _():
            for late in range(1, planes + 1):
                far_start(0, 1, late)
            rim_spread(0)

        @pl.when(index == 2)
        def _():
            for late in (planes + 1, 0):
                when_far(far_start, 0)(late)

        conv_finish(plane)

    inner_slots(functools.partial(gather_forward, 0, 1))
    inner_slots(functools.partial(gather_finish, 0, 1))
    inner_slots(split_far)
    copy_near(1, planes)
    other_copy(0).wait_recv()
    load_copy(3).wait()
    other_copy(1).start()
    build_moved(1, flat_rows(other2))

    @pl.loop(1, planes - 1)
    def _(plane):
        send_result(plane)

    def second_part(flow):
        weight_part(0, flow)
        wide_copy(0, flow).start()

    @pl.loop(0, 2)
    def _(flow):
        second_part(flow)

        @pl.when(flow == 0)
        def _():
            for slot in (planes + 1, 0):
                when_exists(gather_forward, 0, 0)(slot)
                when_far(gather_forward, 0)(slot)

    for slot in (planes + 1, 0):
        when_exists(gather_finish, 0, 0)(slot)
        when_far(gather_finish, 0)(slot)
        split_full(slot)
        split_far(slot)
        copy_near(slot, 1)
    for slot in (planes + 1, 0):
        when_exists(slot_sent, 0, 0)(slot)
    slots_loop(when_far(gather_sent, 0))
    tell(free_sem)

    @pl.loop(0, 2)
    def _(index):
        plane = (index + planes - 1) % planes
        conv_step(plane)
        conv_finish(plane)
        send_result(plane)

        @pl.when(index == 0)
        def _():
            pl.semaphore_wait(free_sem, 1 + chips + rims)
            for slot in range(2, planes):
                send_pair(1, slot)

        send_pair(1, plane + 1)

    rim_start(1)
    wide_event(0, 0)

    @pl.loop(2, 6)
    def _(flow):
        second_part(flow)

        @pl.when(flow == 3)
        def _():
            wide_event(0, 1)

            @pl.loop(2, planes)
            def _(slot):
                gather_forward(1, 0, slot)

        @pl.when(flow == 4)
        def _():
            for slot in (*range(2, planes + 1), 1):
                far_start(1, 1, slot)

    wide_event(0, 2)
    build_moved(0, cube_rows(raw_second))
    rim_take(1)
    rim_spread(1)
    wide_event(0, 3)
    for slot in (planes, 1):
        gather_forward(1, 0, slot)
    other_copy(1).wait_recv()
    build_moved(1, cube_rows(other1))
    wide_event(0, 4)
    for slot in (planes + 1, 0):
        when_far(far_start, 1)(slot)
    inner_slots(functools.partial(gather_forward, 1, 1))
    inner_slots(functools.partial(gather_finish, 1, 0))
    inner_slots(split_full)
    copy_near(1, planes)
    inner_slots(functools.partial(gather_finish, 1, 1))
    inner_slots(split_far)

    @pl.loop(0, 6)
    def _(flow):
        weight_part(1, flow)
        wide_copy(1, flow).start()

        @pl.when(flow == 0)
        def _():
            wide_event(0, 5)
            for slot in (planes + 1, 0):
                when_exists(gather_forward, 1, 0)(slot)
                when_far(gather_forward, 1)(slot)

        @pl.when(flow == 1)
        def _():
            for slot in (planes + 1, 0):
                when_exists(gather_finish, 1, 0)(slot)
                when_far(gather_finish, 1)(slot)
                split_full(slot)
                split_far(slot)
                copy_near(slot, 1)

        @pl.when(flow == 3)
        def _():
            wide_event(1, 0)

        @pl.when(flow == 5)
        def _():
            wide_event(1, 1)

    split_taps(weight1_ref)
    wide_event(1, 2)
    for flow in range(5):
        deep_event(0, flow)

    @pl.loop(0, planes)
    def _(plane):
        conv_plane(plane)

        def finish(start, value):
            raw_out[plane, pl.ds(start, 32), :] = value

        conv_sum(finish)
        for index in range(min(planes, 6)):
            @pl.when(plane == index)
            def _():
                for layer, kind, flow in EVENTS[index]:
                    (wide_event, deep_event)[kind](layer, flow)

    result = pltpu.make_async_copy(raw_out, grad_ref, load_sem.at[0])
    result.start()
    for late in [*EVENTS[min(planes, 6) : 6], EVENTS[6]]:
        for layer, kind, flow in late:
            (wide_event, deep_event)[kind](layer, flow)
    result.wait()
    for flow in range(6):
        store_copy(1, flow).wait()
    slots_loop(when_exists(slot_sent, 1, 0))
    slots_loop(when_far(gather_sent, 1))
    rim_sent(1)
    for layer in range(2):
        other_copy(layer).wait_send()
        for flow in range(6):
            wide_copy(layer, flow).wait_send()
            for j in range(1, members):
                deep_copy(layer, flow, j).wait_send()


def per_device(saved_input, pre_first, pre_second, out_grad, weight_first, weight_second):
    channels, planes, area = saved_input.shape
    total = weight_first.shape[2]
    slabs, chans = lax.axis_size("slab"), lax.axis_size("chan")
    side = math.isqrt(area)
    block = total // slabs
    groups = 128 // block
    steps = 9 * channels
    rows = steps // groups // 2
    width = planes * area
    wide = (planes + 2) * area
    chips, members, half = chans // 2, slabs // 4, total // 2
    dims = (slabs, chans, total, planes, area, side)
    hbm = pl.BlockSpec(memory_space=pl.ANY)
    cube = pltpu.VMEM((planes, channels, area), F32)
    flat = pltpu.VMEM((channels, width), F32)
    dma = pltpu.SemaphoreType.DMA
    out_part = jax.ShapeDtypeStruct((3, steps, block), F32)
    input_grad, first, second = pl.pallas_call(
        functools.partial(mega, dims),
        out_shape=(jax.ShapeDtypeStruct((planes, channels, area), F32), out_part, out_part),
        in_specs=[hbm] * 6,
        out_specs=(hbm, hbm, hbm),
        scratch_shapes=[
            *[cube] * 3,
            *[flat] * 3,
            cube,
            pltpu.VMEM((total, wide), F32),
            pltpu.VMEM((half, wide), F32),
            *[pltpu.VMEM((total, wide), BF16)] * 2,
            *[pltpu.VMEM((2, half, wide), BF16)] * 2,
            *[pltpu.VMEM((2, steps, width), BF16)] * 2,
            *[pltpu.VMEM((3, steps, total), BF16)] * 2,
            pltpu.VMEM((2, steps // 2, total), F32),
            pltpu.VMEM((steps // 2, half), F32),
            pltpu.VMEM((steps, area), F32),
            *[pltpu.VMEM((6, 2, members, rows, 128), F32)] * 2,
            *[pltpu.VMEM((6, members, rows, 128), F32)] * 2,
            *[pltpu.VMEM((6, max(members - 1, 1), rows, 128), F32)] * 2,
            pltpu.VMEM((6, steps // 2, block), F32),
            dma((4,)),
            dma((2,)),
            *[dma((2, 2, planes + 2, 2 * chips))] * 2,
            *[dma((2, 2))] * 2,
            *[dma((2, planes + 2))] * 2,
            *[dma((2,))] * 2,
            *[dma((2, 6))] * 2,
            *[dma((2, 6, max(members - 1, 1)))] * 2,
            dma((2, 6)),
            pltpu.SemaphoreType.REGULAR,
            pltpu.SemaphoreType.REGULAR((planes,)),
        ],
        compiler_params=pltpu.CompilerParams(
            collective_id=0, has_side_effects=True, vmem_limit_bytes=67043328
        ),
        name="backward",
    )(
        *(value.transpose(1, 0, 2) for value in (saved_input, pre_first, pre_second, out_grad)),
        weight_first.reshape(3, steps, total),
        weight_second.reshape(3, steps, total),
    )
    scale = math.sqrt(planes * slabs * area)

    def finish(summed):
        return summed.reshape(27, channels, block) / scale

    return input_grad.transpose(1, 0, 2), finish(first), finish(second)


def solution(mesh):
    in_specs = (
        P("chan", "slab", None),
        P("chan", "slab", None),
        P("chan", "slab", None),
        P("chan", "slab", None),
        P(None, "chan", None),
        P(None, "chan", None),
    )
    out_specs = (P("chan", "slab", None), P(None, "chan", "slab"), P(None, "chan", "slab"))
    return jax.shard_map(
        per_device, mesh=mesh, in_specs=in_specs, out_specs=out_specs, check_vma=False
    )
```

```python
import functools
import math

import jax
import jax.numpy as jnp
from jax import lax
from jax.experimental import pallas as pl
from jax.experimental.pallas import tpu as pltpu
from jax.sharding import PartitionSpec as P

F32 = jnp.float32
BF16 = jnp.bfloat16
MESH = pl.DeviceIdType.MESH
STEPS = (-1, 0, 1)
EVENTS = (
    ((1, 0, 3), (0, 1, 5)),
    ((1, 1, 0),),
    ((1, 0, 4), (1, 1, 1)),
    ((1, 0, 5),),
    ((1, 1, 2),),
    ((1, 1, 3),),
    ((1, 1, 4), (1, 1, 5)),
)
IN_PLANE = [(row_step, col_step) for row_step in STEPS for col_step in STEPS]


def silu_slope(values):
    sigma = jax.nn.sigmoid(values)
    return sigma * (1.0 + values * (1.0 - sigma))


def halves(value):
    high = value.astype(BF16)
    return high, (value - high.astype(F32)).astype(BF16)


def dot_nn(left, right):
    return lax.dot_general(left, right, (((1,), (0,)), ((), ())), preferred_element_type=F32)


def dot_nt(left, right):
    return lax.dot_general(left, right, (((1,), (1,)), ((), ())), preferred_element_type=F32)


def mega(
    dims,
    saved_hbm, first_hbm, second_hbm, out_hbm, weight1_ref, weight2_ref,
    grad_ref, out1_ref, out2_ref,
    raw_second, raw_first, raw_out, sent, hidden, other2, other1,
    full, far, full_h, full_l, near_h, near_l, moved_h, moved_l, taps_h, taps_l,
    stage, raw, mixed, part2, part1, gotw2, gotw1, gotd2, gotd1, final,
    load_sem, stage_sem, gather_send, gather_recv, rim_send, rim_recv, pair_send, pair_recv,
    other_send, other_recv, wide_send, wide_recv, deep_send, deep_recv, store_sem, free_sem, slot_sem,
):
    slabs, chans, total, planes, area, side = dims
    channels = total // chans
    block = total // slabs
    groups = 128 // block
    rows = len(IN_PLANE) * channels // groups // 2
    chips = chans // 2
    members = slabs // 4
    owned = 2 * block
    half = total // 2
    width = planes * area
    wide = (planes + 2) * area
    steps = 9 * channels
    lump = steps // 2

    slab = lax.axis_index("slab")
    chan = lax.axis_index("chan")
    chip, core = chan // 2, chan % 2
    deep, across = slab // 2, slab % 2
    parity, member = deep % 2, deep // 2
    pair = slab + 2 - 4 * parity
    beside = slab + 1 - 2 * across
    partner = chip * 2 + 1 - core

    def kind_of(index):
        return (index * slabs // (2 * chans)) % 2

    takes = kind_of(chan) == parity
    gives = kind_of(chan) != parity

    def far_chan(j):
        return ((chip + j) % chips) * 2 + core

    def near_chan(j):
        return ((chip + chips - j) % chips) * 2 + core

    def crossed_chan(j):
        return ((chip + chips - j) % chips) * 2 + 1 - core

    def deep_slab(j):
        return 2 * (2 * ((member + j) % members) + parity) + across

    has_left = slab > 0
    has_right = slab < slabs - 1
    rims = jnp.minimum(slab, 1) + jnp.minimum(slabs - 1 - slab, 1)

    def signal(semaphore, **target):
        pl.semaphore_signal(semaphore, inc=1, device_id=target, device_id_type=MESH)

    def tell(semaphore):
        for j in range(1, chips):
            signal(semaphore, chan=far_chan(j))
        signal(semaphore, chan=partner)
        signal(semaphore, slab=pair)

        @pl.when(has_left)
        def _():
            signal(semaphore, slab=slab - 1)

        @pl.when(has_right)
        def _():
            signal(semaphore, slab=slab + 1)

    def load_copy(index):
        source = (second_hbm, out_hbm, first_hbm, saved_hbm)[index]
        target = (raw_second, raw_out, raw_first, raw_second)[index]
        return pltpu.make_async_copy(source, target, load_sem.at[index])

    def stage_copy(weight_ref, piece):
        source = weight_ref.at[piece // 2, pl.ds(piece % 2 * lump, lump)]
        return pltpu.make_async_copy(source, stage.at[piece % 2], stage_sem.at[piece % 2])

    for index in range(3):
        load_copy(index).start()
    stage_copy(weight2_ref, 0).start()
    stage_copy(weight2_ref, 1).start()

    barrier = pltpu.get_barrier_semaphore()
    tell(barrier)
    signal(barrier, slab=beside)
    for j in range(1, members):
        signal(barrier, slab=deep_slab(j))

    def chan_rows(index):
        return pl.ds(pl.multiple_of(index * channels, channels), channels)

    def far_rows(index):
        start = index * channels
        group = start // (2 * owned)
        inside = start - (2 * group + kind_of(index)) * owned
        return pl.ds(pl.multiple_of(group * owned + inside, channels), channels)

    def lanes(slot, count=1):
        return pl.ds(pl.multiple_of(slot * area, area), count * area)

    mine = chan_rows(chan)

    def exists(kind, slot):
        base = (slab, pair)[kind]
        return (slot + base > 0) & (slot - (planes + 1) + base < slabs - 1)

    def rim_copy(layer, toward, source):
        return pltpu.make_async_remote_copy(
            src_ref=source,
            dst_ref=full.at[mine, lanes((0, planes + 1)[toward])],
            send_sem=rim_send.at[layer, toward],
            recv_sem=rim_recv.at[layer, toward],
            device_id={"slab": (slab + 1, slab - 1)[toward]},
            device_id_type=MESH,
        )

    def rim_start(layer):
        @pl.when(has_right)
        def _():
            rim_copy(layer, 0, sent.at[:, lanes(planes - 1)]).start()

        @pl.when(has_left)
        def _():
            rim_copy(layer, 1, sent.at[:, lanes(0)]).start()

    def rim_sent(layer):
        @pl.when(has_right)
        def _():
            rim_copy(layer, 0, sent.at[:, lanes(0)]).wait_send()

        @pl.when(has_left)
        def _():
            rim_copy(layer, 1, sent.at[:, lanes(0)]).wait_send()

    def pair_copy(layer, slot, source):
        return pltpu.make_async_remote_copy(
            src_ref=source,
            dst_ref=far.at[far_rows(chan), lanes(slot)],
            send_sem=pair_send.at[layer, slot],
            recv_sem=pair_recv.at[layer, slot],
            device_id={"slab": pair},
            device_id_type=MESH,
        )

    def other_copy(layer):
        return pltpu.make_async_remote_copy(
            src_ref=(hidden, raw_second)[layer],
            dst_ref=(other2, other1)[layer],
            send_sem=other_send.at[layer],
            recv_sem=other_recv.at[layer],
            device_id={"slab": pair},
            device_id_type=MESH,
        )

    def gather_copy(layer, kind, slot, source, owner, index, target):
        where = (chan_rows, far_rows)[kind](owner)
        return pltpu.make_async_remote_copy(
            src_ref=source,
            dst_ref=(full, far)[kind].at[where, lanes(slot)],
            send_sem=gather_send.at[layer, kind, slot, index],
            recv_sem=gather_recv.at[layer, kind, slot, index],
            device_id={"chan": target},
            device_id_type=MESH,
        )

    def held(kind, owner, slot):
        if kind == 0:
            return full.at[chan_rows(owner), lanes(slot)]
        return far.at[far_rows(owner), lanes(slot)]

    def guard(kind, owner):
        if kind == 0:
            return lambda action: action()
        return pl.when(kind_of(owner) == parity)

    def gather_start(layer, kind, slot, source):
        for j in range(1, chips):
            gather_copy(layer, kind, slot, source, chan, j, far_chan(j)).start()
        gather_copy(layer, kind, slot, source, chan, 0, partner).start()

    def gather_forward(layer, kind, slot):
        for j in range(1, chips):
            owner = near_chan(j)

            @guard(kind, owner)
            def _():
                view = held(kind, owner, slot)
                gather_copy(layer, kind, slot, view, owner, j, partner).wait_recv()
                gather_copy(layer, kind, slot, view, owner, chips + j, partner).start()

    def gather_finish(layer, kind, slot):
        @guard(kind, partner)
        def _():
            gather_copy(layer, kind, slot, held(kind, partner, slot), partner, 0, partner).wait_recv()

        for j in range(1, chips):
            owner = crossed_chan(j)

            @guard(kind, owner)
            def _():
                view = held(kind, owner, slot)
                gather_copy(layer, kind, slot, view, owner, chips + j, partner).wait_recv()

    def gather_sent(layer, kind, slot):
        @guard(kind, chan)
        def _():
            for index in range(chips):
                view = held(kind, chan, slot)
                gather_copy(layer, kind, slot, view, chan, index, partner).wait_send()

        for j in range(1, chips):
            owner = near_chan(j)

            @guard(kind, owner)
            def _():
                view = held(kind, owner, slot)
                gather_copy(layer, kind, slot, view, owner, chips + j, partner).wait_send()

    def slots_loop(action):
        @pl.loop(0, planes + 2)
        def _(index):
            action((index + 1) % (planes + 2))

    def when_exists(action, layer, kind):
        def run(slot):
            @pl.when(exists(kind, slot))
            def _():
                action(layer, kind, slot)

        return run

    def send_slot(layer, slot):
        gather_start(layer, 0, slot, sent.at[:, lanes(slot - 1)])

    def send_pair(layer, slot):
        @pl.when(gives)
        def _():
            pair_copy(layer, slot, sent.at[:, lanes(slot - 1)]).start()

    def rim_take(layer):
        for toward in range(2):
            slot = (0, planes + 1)[toward]

            @pl.when((has_left, has_right)[toward])
            def _():
                view = full.at[mine, lanes(slot)]
                rim_copy(layer, toward, view).wait_recv()

                @pl.when(gives)
                def _():
                    pair_copy(layer, slot, view).start()

    def rim_spread(layer):
        for slot in (planes + 1, 0):

            @pl.when(exists(0, slot))
            def _():
                gather_start(layer, 0, slot, full.at[mine, lanes(slot)])

    def far_start(layer, kind, slot):
        @pl.when(takes)
        def _():
            view = held(1, chan, slot)
            pair_copy(layer, slot, view).wait_recv()
            gather_start(layer, 1, slot, view)

    def pair_sent(layer, slot):
        @pl.when(gives)
        def _():
            pair_copy(layer, slot, sent.at[:, lanes(0)]).wait_send()

    def slot_sent(layer, kind, slot):
        gather_sent(layer, 0, slot)
        pair_sent(layer, slot)

    def split_rows(source, start, high_ref, low_ref, target, slot):
        high, low = halves(source[pl.ds(start, 32), lanes(slot)])
        high_ref[pl.ds(target, 32), lanes(slot)] = high
        low_ref[pl.ds(target, 32), lanes(slot)] = low

    def split_full(slot):
        @pl.when(exists(0, slot))
        def _():
            @pl.loop(0, total // 32)
            def _(index):
                start = pl.multiple_of(index * 32, 32)
                split_rows(full, start, full_h, full_l, start, slot)

        @pl.when(jnp.logical_not(exists(0, slot)))
        def _():
            @pl.loop(0, total // 32)
            def _(index):
                where = pl.ds(pl.multiple_of(index * 32, 32), 32)
                full_h[where, lanes(slot)] = jnp.zeros((32, area), BF16)
                full_l[where, lanes(slot)] = jnp.zeros((32, area), BF16)

    def copy_near(slot, count):
        @pl.loop(0, half // 32)
        def _(index):
            start = pl.multiple_of(index * 32, 32)
            group = start // owned
            where = pl.ds(pl.multiple_of(start + (group + parity) * owned, 32), 32)
            near_h[0, pl.ds(start, 32), lanes(slot, count)] = full_h[where, lanes(slot, count)]
            near_l[0, pl.ds(start, 32), lanes(slot, count)] = full_l[where, lanes(slot, count)]

    def split_far(slot):
        @pl.when(exists(1, slot))
        def _():
            @pl.loop(0, half // 32)
            def _(index):
                start = pl.multiple_of(index * 32, 32)
                split_rows(far, start, near_h.at[1], near_l.at[1], start, slot)

        @pl.when(jnp.logical_not(exists(1, slot)))
        def _():
            @pl.loop(0, half // 32)
            def _(index):
                where = pl.ds(pl.multiple_of(index * 32, 32), 32)
                near_h[1, where, lanes(slot)] = jnp.zeros((32, area), BF16)
                near_l[1, where, lanes(slot)] = jnp.zeros((32, area), BF16)

    cells = lax.broadcasted_iota(jnp.int32, (1, area), 1)
    row_ids, col_ids = cells // side, cells % side

    def mask_of(row_step, col_step):
        valid = (
            (row_ids + row_step >= 0)
            & (row_ids + row_step < side)
            & (col_ids + col_step >= 0)
            & (col_ids + col_step < side)
        )
        return jnp.where(valid, 1.0, 0.0).astype(F32)

    def shifted(value, row_step, col_step):
        if row_step == 0 and col_step == 0:
            return value
        shift = (-(row_step * side + col_step)) % area
        return pltpu.roll(value, shift, 1) * mask_of(row_step, col_step)

    def flat_rows(source):
        return lambda plane, where: source[where, lanes(plane)]

    def cube_rows(source):
        return lambda plane, where: source[plane, where, :]

    def build_moved(piece, source):
        @pl.loop(0, planes)
        def _(plane):
            @pl.loop(0, channels // 32)
            def _(index):
                start = pl.multiple_of(index * 32, 32)
                value = source(plane, pl.ds(start, 32))
                for tap, (row_step, col_step) in enumerate(IN_PLANE):
                    high, low = halves(shifted(value, row_step, col_step))
                    where = pl.ds(pl.multiple_of(tap * channels + start, 32), 32)
                    moved_h[piece, where, lanes(plane)] = high
                    moved_l[piece, where, lanes(plane)] = low

    def split_taps(weight_ref):
        for piece in range(6):
            stage_copy(weight_ref, piece).wait()

            @pl.loop(0, lump // 48)
            def _(index):
                start = pl.multiple_of(index * 48, 48)
                high, low = halves(stage[piece % 2, pl.ds(start, 48), :])
                where = pl.ds(pl.multiple_of(piece % 2 * lump + start, 48), 48)
                taps_h[piece // 2, where, :] = high
                taps_l[piece // 2, where, :] = low

            if piece < 4:
                stage_copy(weight_ref, piece + 2).start()

    parts, gotw, gotd = (part2, part1), (gotw2, gotw1), (gotd2, gotd1)
    outs = (out2_ref, out1_ref)

    def wide_copy(layer, flow):
        return pltpu.make_async_remote_copy(
            src_ref=parts[layer].at[flow, 1 - across],
            dst_ref=gotw[layer].at[flow],
            send_sem=wide_send.at[layer, flow],
            recv_sem=wide_recv.at[layer, flow],
            device_id={"slab": beside},
            device_id_type=MESH,
        )

    def deep_copy(layer, flow, j):
        return pltpu.make_async_remote_copy(
            src_ref=parts[layer].at[flow, across, (member + j) % members],
            dst_ref=gotd[layer].at[flow, j - 1],
            send_sem=deep_send.at[layer, flow, j - 1],
            recv_sem=deep_recv.at[layer, flow, j - 1],
            device_id={"slab": deep_slab(j)},
            device_id_type=MESH,
        )

    def store_copy(layer, flow):
        depth, where = (flow // 2 + 1) % 3, pl.ds(flow % 2 * lump, lump)
        return pltpu.make_async_copy(
            final.at[flow], outs[layer].at[depth, where], store_sem.at[layer, flow]
        )

    def rows_loop(action):
        if rows % 72:
            action(0, rows)
        else:

            @pl.loop(0, rows // 72)
            def _(part):
                action(pl.multiple_of(part * 72, 8), 72)

    def wide_event(layer, flow):
        wide_copy(layer, flow).wait_recv()
        for j in [*range(1, members), 0]:
            index = (member + j) % members

            def add(start, count):
                where = pl.ds(start, count)
                parts[layer][flow, across, index, where] = (
                    parts[layer][flow, across, index, where] + gotw[layer][flow, index, where]
                )

            rows_loop(add)
            if j:
                deep_copy(layer, flow, j).start()

    def deep_event(layer, flow):
        for j in range(1, members):
            deep_copy(layer, flow, j).wait_recv()
        if layer:
            store_copy(0, flow).wait()

        def add(start, count):
            where = pl.ds(start, count)
            value = parts[layer][flow, across, member, where]
            for j in range(1, members):
                value += gotd[layer][flow, j - 1, where]
            for v in range(groups):
                piece = pltpu.roll(value, (128 - v * block) % 128, 1) if v else value
                final[flow, pl.ds(v * rows + start, count), :] = piece[:, :block]

        rows_loop(add)
        store_copy(layer, flow).start()

    def pack(layer, flow):
        lane = lax.broadcasted_iota(jnp.int32, (1, 128), 1) // block

        def move(start, count):
            for tile in range(half // 128):
                pieces = [
                    raw[pl.ds(v * rows + start, count), pl.ds(tile * 128, 128)]
                    for v in range(groups)
                ]
                for u in range(groups):
                    value = None
                    for v in range(groups):
                        piece = pieces[v]
                        if u != v:
                            piece = pltpu.roll(piece, ((v - u) * block) % 128, 1)
                        value = piece if value is None else jnp.where(lane == v, piece, value)
                    owner = tile * groups + u
                    parts[layer][flow, owner % 2, owner // 2, pl.ds(start, count)] = value

        rows_loop(move)

    def weight_part(layer, flow):
        depth = (flow // 2 + 1) % 3
        window = lanes(2 - depth, planes)
        where = pl.ds(pl.multiple_of(flow % 2 * lump, lump), lump)
        value = jnp.zeros((lump, half), F32)
        for piece in range(2):
            value += dot_nt(moved_h[piece, where, :], near_h[piece, :, window])
            value += dot_nt(moved_h[piece, where, :], near_l[piece, :, window])
            value += dot_nt(moved_l[piece, where, :], near_h[piece, :, window])
        raw[...] = value
        pack(layer, flow)

    def conv_plane(plane):
        value = jnp.zeros((steps, area), F32)
        for depth in range(3):
            window = lanes(plane + 2 - depth)
            value += dot_nn(taps_h[depth], full_h[:, window])
            value += dot_nn(taps_h[depth], full_l[:, window])
            value += dot_nn(taps_l[depth], full_h[:, window])
        mixed[...] = value

    def conv_sum(finish):
        @pl.loop(0, channels // 32)
        def _(index):
            start = pl.multiple_of(index * 32, 32)
            value = jnp.zeros((32, area), F32)
            for tap, (row_step, col_step) in enumerate(IN_PLANE):
                where = pl.ds(pl.multiple_of(tap * channels + start, 32), 32)
                value += shifted(mixed[where, :], -row_step, -col_step)
            finish(start, value)

    def each_plane(action):
        @pl.loop(0, planes)
        def _(plane):
            @pl.loop(0, channels // 32)
            def _(index):
                action(plane, pl.ds(pl.multiple_of(index * 32, 32), 32))

    load_copy(0).wait()
    load_copy(1).wait()

    def make_sent(plane, where):
        sent[where, lanes(plane)] = raw_out[plane, where, :] * silu_slope(raw_second[plane, where, :])

    each_plane(make_sent)
    load_copy(3).start()
    load_copy(2).wait()

    def make_hidden(plane, where):
        value = raw_first[plane, where, :]
        hidden[where, lanes(plane)] = value * jax.nn.sigmoid(value)

    each_plane(make_hidden)
    pl.semaphore_wait(barrier, 1 + members + chips + rims)
    rim_start(0)
    for slot in range(1, 4):
        send_slot(0, slot)
    for slot in range(1, planes + 1):
        send_pair(0, slot)

    def keep_sent(plane, where):
        target = pl.ds(pl.multiple_of(chan * channels + where.start, 32), 32)
        full[target, lanes(plane + 1)] = sent[where, lanes(plane)]

    each_plane(keep_sent)
    split_taps(weight2_ref)
    stage_copy(weight1_ref, 0).start()
    stage_copy(weight1_ref, 1).start()
    for slot in range(4, planes + 1):
        send_slot(0, slot)
    rim_take(0)
    other_copy(0).start()
    build_moved(0, flat_rows(hidden))
    for slot in (1, 2, 3):
        gather_forward(0, 0, slot)
    for slot in (1, 2):
        gather_finish(0, 0, slot)
        split_full(slot)

    def when_far(action, layer):
        return when_exists(action, layer, 1)

    def inner_slots(action):
        @pl.loop(1, planes + 1)
        def _(slot):
            action(slot)

    def conv_step(plane):
        slot_sent(0, 0, plane + 1)
        for j in range(1, chips):
            signal(slot_sem.at[plane], chan=far_chan(j))
        signal(slot_sem.at[plane], chan=partner)
        conv_plane(plane)

    def conv_finish(plane):
        @pl.when((plane == 0) & has_left)
        def _():
            rim_copy(0, 1, sent.at[:, lanes(0)]).wait_send()

        @pl.when((plane == planes - 1) & has_right)
        def _():
            rim_copy(0, 0, sent.at[:, lanes(0)]).wait_send()

        def finish(start, value):
            where = pl.ds(start, 32)
            target = pl.ds(pl.multiple_of(chan * channels + start, 32), 32)
            value = value * silu_slope(raw_first[plane, where, :])
            sent[where, lanes(plane)] = value
            full[target, lanes(plane + 1)] = value

        conv_sum(finish)

    def send_result(plane):
        pl.semaphore_wait(slot_sem.at[plane], chips)
        send_slot(1, plane + 1)

    @pl.loop(0, planes - 2)
    def _(index):
        plane = index + 1
        slot = index + 3
        gather_finish(0, 0, slot)
        split_full(slot)
        conv_step(plane)

        @pl.when(index < planes - 3)
        def _():
            gather_forward(0, 0, slot + 1)

        @pl.when(index == 0)
        def _():
            for late in range(1, planes + 1):
                far_start(0, 1, late)
            rim_spread(0)

        @pl.when(index == 2)
        def _():
            for late in (planes + 1, 0):
                when_far(far_start, 0)(late)

        conv_finish(plane)

    inner_slots(functools.partial(gather_forward, 0, 1))
    inner_slots(functools.partial(gather_finish, 0, 1))
    inner_slots(split_far)
    copy_near(1, planes)
    other_copy(0).wait_recv()
    load_copy(3).wait()
    other_copy(1).start()
    build_moved(1, flat_rows(other2))

    @pl.loop(1, planes - 1)
    def _(plane):
        send_result(plane)

    def second_part(flow):
        weight_part(0, flow)
        wide_copy(0, flow).start()

    @pl.loop(0, 2)
    def _(flow):
        second_part(flow)

        @pl.when(flow == 0)
        def _():
            for slot in (planes + 1, 0):
                when_exists(gather_forward, 0, 0)(slot)
                when_far(gather_forward, 0)(slot)

    for slot in (planes + 1, 0):
        when_exists(gather_finish, 0, 0)(slot)
        when_far(gather_finish, 0)(slot)
        split_full(slot)
        split_far(slot)
        copy_near(slot, 1)
    for slot in (planes + 1, 0):
        when_exists(slot_sent, 0, 0)(slot)
    slots_loop(when_far(gather_sent, 0))
    tell(free_sem)

    @pl.loop(0, 2)
    def _(index):
        plane = (index + planes - 1) % planes
        conv_step(plane)
        conv_finish(plane)
        send_result(plane)

        @pl.when(index == 0)
        def _():
            pl.semaphore_wait(free_sem, 1 + chips + rims)
            for slot in range(2, planes):
                send_pair(1, slot)

        send_pair(1, plane + 1)

    rim_start(1)
    wide_event(0, 0)

    @pl.loop(2, 6)
    def _(flow):
        second_part(flow)

        @pl.when(flow == 3)
        def _():
            wide_event(0, 1)

            @pl.loop(2, planes)
            def _(slot):
                gather_forward(1, 0, slot)

        @pl.when(flow == 4)
        def _():
            for slot in (*range(2, planes + 1), 1):
                far_start(1, 1, slot)

    wide_event(0, 2)
    build_moved(0, cube_rows(raw_second))
    rim_take(1)
    rim_spread(1)
    wide_event(0, 3)
    for slot in (planes, 1):
        gather_forward(1, 0, slot)
    other_copy(1).wait_recv()
    build_moved(1, cube_rows(other1))
    wide_event(0, 4)
    for slot in (planes + 1, 0):
        when_far(far_start, 1)(slot)
    inner_slots(functools.partial(gather_forward, 1, 1))
    inner_slots(functools.partial(gather_finish, 1, 0))
    inner_slots(split_full)
    copy_near(1, planes)
    inner_slots(functools.partial(gather_finish, 1, 1))
    inner_slots(split_far)

    @pl.loop(0, 6)
    def _(flow):
        weight_part(1, flow)
        wide_copy(1, flow).start()

        @pl.when(flow == 0)
        def _():
            wide_event(0, 5)
            for slot in (planes + 1, 0):
                when_exists(gather_forward, 1, 0)(slot)
                when_far(gather_forward, 1)(slot)

        @pl.when(flow == 1)
        def _():
            for slot in (planes + 1, 0):
                when_exists(gather_finish, 1, 0)(slot)
                when_far(gather_finish, 1)(slot)
                split_full(slot)
                split_far(slot)
                copy_near(slot, 1)

        @pl.when(flow == 3)
        def _():
            wide_event(1, 0)

        @pl.when(flow == 5)
        def _():
            wide_event(1, 1)

    split_taps(weight1_ref)
    wide_event(1, 2)
    for flow in range(5):
        deep_event(0, flow)

    @pl.loop(0, planes)
    def _(plane):
        conv_plane(plane)

        def finish(start, value):
            raw_out[plane, pl.ds(start, 32), :] = value

        conv_sum(finish)
        for index in range(min(planes, 6)):
            @pl.when(plane == index)
            def _():
                for layer, kind, flow in EVENTS[index]:
                    (wide_event, deep_event)[kind](layer, flow)

    result = pltpu.make_async_copy(raw_out, grad_ref, load_sem.at[0])
    result.start()
    for late in [*EVENTS[min(planes, 6) : 6], EVENTS[6]]:
        for layer, kind, flow in late:
            (wide_event, deep_event)[kind](layer, flow)
    result.wait()
    for flow in range(6):
        store_copy(1, flow).wait()
    slots_loop(when_exists(slot_sent, 1, 0))
    slots_loop(when_far(gather_sent, 1))
    rim_sent(1)
    for layer in range(2):
        other_copy(layer).wait_send()
        for flow in range(6):
            wide_copy(layer, flow).wait_send()
            for j in range(1, members):
                deep_copy(layer, flow, j).wait_send()


def per_device(saved_input, pre_first, pre_second, out_grad, weight_first, weight_second):
    channels, planes, area = saved_input.shape
    total = weight_first.shape[2]
    slabs, chans = lax.axis_size("slab"), lax.axis_size("chan")
    side = math.isqrt(area)
    block = total // slabs
    groups = 128 // block
    steps = 9 * channels
    rows = steps // groups // 2
    width = planes * area
    wide = (planes + 2) * area
    chips, members, half = chans // 2, slabs // 4, total // 2
    dims = (slabs, chans, total, planes, area, side)
    hbm = pl.BlockSpec(memory_space=pl.ANY)
    cube = pltpu.VMEM((planes, channels, area), F32)
    flat = pltpu.VMEM((channels, width), F32)
    dma = pltpu.SemaphoreType.DMA
    out_part = jax.ShapeDtypeStruct((3, steps, block), F32)
    input_grad, first, second = pl.pallas_call(
        functools.partial(mega, dims),
        out_shape=(jax.ShapeDtypeStruct((planes, channels, area), F32), out_part, out_part),
        in_specs=[hbm] * 6,
        out_specs=(hbm, hbm, hbm),
        scratch_shapes=[
            *[cube] * 3,
            *[flat] * 3,
            cube,
            pltpu.VMEM((total, wide), F32),
            pltpu.VMEM((half, wide), F32),
            *[pltpu.VMEM((total, wide), BF16)] * 2,
            *[pltpu.VMEM((2, half, wide), BF16)] * 2,
            *[pltpu.VMEM((2, steps, width), BF16)] * 2,
            *[pltpu.VMEM((3, steps, total), BF16)] * 2,
            pltpu.VMEM((2, steps // 2, total), F32),
            pltpu.VMEM((steps // 2, half), F32),
            pltpu.VMEM((steps, area), F32),
            *[pltpu.VMEM((6, 2, members, rows, 128), F32)] * 2,
            *[pltpu.VMEM((6, members, rows, 128), F32)] * 2,
            *[pltpu.VMEM((6, max(members - 1, 1), rows, 128), F32)] * 2,
            pltpu.VMEM((6, steps // 2, block), F32),
            dma((4,)),
            dma((2,)),
            *[dma((2, 2, planes + 2, 2 * chips))] * 2,
            *[dma((2, 2))] * 2,
            *[dma((2, planes + 2))] * 2,
            *[dma((2,))] * 2,
            *[dma((2, 6))] * 2,
            *[dma((2, 6, max(members - 1, 1)))] * 2,
            dma((2, 6)),
            pltpu.SemaphoreType.REGULAR,
            pltpu.SemaphoreType.REGULAR((planes,)),
        ],
        compiler_params=pltpu.CompilerParams(
            collective_id=0, has_side_effects=True, vmem_limit_bytes=67043328
        ),
        name="backward",
    )(
        *(value.transpose(1, 0, 2) for value in (saved_input, pre_first, pre_second, out_grad)),
        weight_first.reshape(3, steps, total),
        weight_second.reshape(3, steps, total),
    )
    scale = math.sqrt(planes * slabs * area)

    def finish(summed):
        turned = lax.optimization_barrier(summed.reshape(27, channels, block).transpose(0, 2, 1))
        return (turned / scale).transpose(0, 2, 1)

    return input_grad.transpose(1, 0, 2), finish(first), finish(second)


def solution(mesh):
    in_specs = (
        P("chan", "slab", None),
        P("chan", "slab", None),
        P("chan", "slab", None),
        P("chan", "slab", None),
        P(None, "chan", None),
        P(None, "chan", None),
    )
    out_specs = (P("chan", "slab", None), P(None, "chan", "slab"), P(None, "chan", "slab"))
    return jax.shard_map(
        per_device, mesh=mesh, in_specs=in_specs, out_specs=out_specs, check_vma=False
    )
```
